128 devices in a mesh: energy: 16 (over y, x), kpt: 8 (over z, core).
Axes of the slice: x: 4, y: 4, z: 4, core: 2. Of those that a mesh axis runs over, the one named last changes fastest.
Arguments:
- density: bfloat16 [64, 8, 128, 3072], P('energy', 'kpt'), may hold values from -6 to 6
- quad_weights: float32 [64, 8], P('energy', 'kpt'), may hold values from 0.022097087 to 0.088388346
- orbital_cells: int32 [128, 3072], replicated, may hold values from 0 to 262143
- fixed_charge: float32 [1024, 128, 256], P('energy', 'kpt'), may hold values from -16 to 16
- gate_mask: int32 [1024, 128, 256], P('energy', 'kpt'), may hold values 0 or 1
- gate_voltage: float32 [1024], P('energy'), may hold values from -1 to 1
Outputs:
- potential: float32 [1024, 128, 256], P('energy', 'kpt')
- band_shift: float32 [64, 8, 128], P('energy', 'kpt')
The draws below stay inside these ranges and needn't reach their ends.
Inputs may be any that keep to these rules, and one draw needn't show every extreme that they name: `orbital_cells`: each entry is s * 128 * 256 + y * 256 + z, a cell of one of the layer's 8 planes.
All inputs are finite; a program needn't handle non-finite values. No bound on the sum of `gate_mask` on one device may be relied on, other than what follows from the above.
Results may differ from the reference program's by a relative error of at most 0.0003.
Values sent between devices are 32-bit elements; how exact they have to be, the bound alone decides.
No kernel may reach another device: no remote copies, remote signals or barrier semaphores. Data moves between devices by JAX's collectives and lax.ppermute only.
A program may use at most 64 MiB of HBM per device.

```python
import math
import jax
import jax.numpy as jnp
from jax import lax

ORBITALS = 3072
SUB = 8
CY = 16
NZ = 256
ITERS = 2
ENERGIES = 64
KPOINTS = 8
LAYERS = 128
NY = 128
CX = 64
GX = 1024


def draw_fixed_charge(key, part):
    blocks_x = GX // CX
    blocks_y = NY // CY
    block_count = blocks_x * blocks_y
    ranking = jax.random.permutation(jax.random.fold_in(key, 12), block_count)
    chosen = (ranking < block_count // 2).astype(jnp.float32)
    phases = jax.random.uniform(jax.random.fold_in(key, 14), (3,), jnp.float32, 0.0, 2.0 * math.pi)
    white_noise = jnp.clip(jax.random.normal(jax.random.fold_in(key, 11), (GX, NY, NZ), jnp.float32), -6.0, 6.0)
    levels = jax.random.uniform(jax.random.fold_in(key, 13), (block_count,), jnp.float32, 1.5, 3.0) * chosen
    block_level = jnp.repeat(jnp.repeat(levels.reshape(blocks_x, blocks_y), CX, axis=0), CY, axis=1)
    plane_pos = (jnp.arange(GX, dtype=jnp.float32) + 0.5) / GX
    column_pos = (jnp.arange(NY, dtype=jnp.float32) + 0.5) / NY
    depth_pos = (jnp.arange(NZ, dtype=jnp.float32) + 0.5) / NZ
    plane_wave = jnp.sin(2.0 * math.pi * plane_pos + phases[0])
    column_wave = jnp.sin(2.0 * math.pi * column_pos + phases[1])
    depth_wave = jnp.sin(2.0 * math.pi * depth_pos + phases[2])
    smooth_field = 1.0 + 0.5 * plane_wave[:, None, None] * depth_wave[None, None, :] + 0.4 * column_wave[None, :, None]
    return (white_noise + block_level[:, :, None] * smooth_field).astype(jnp.float32)


def with_ends(values, stream_key, smallest, largest):
    longest = values.shape.index(max(values.shape))
    spots = []
    for shift in (0, 1):
        where = [jax.random.randint(jax.random.fold_in(stream_key, axis), (), 0, length) for axis, length in enumerate(values.shape)]
        where[longest] = (where[longest] + shift) % values.shape[longest]
        spots.append(tuple(where))
    return values.at[spots[0]].set(smallest).at[spots[1]].set(largest)


def strengthened(entries, rng, source, target, shards_of, factor):
    owner, partner = [(jnp.arange(entries.shape[axis_at]) // (entries.shape[axis_at] // shards_of)).reshape([-1 if axis == axis_at else 1 for axis in range(entries.ndim)]) for axis_at in (source, target)]
    chosen = jax.random.permutation(rng, shards_of)[partner]
    strong = (owner == chosen) | (owner == (partner + shards_of // 2) % shards_of)
    return jnp.where(strong, factor * entries, entries)


def block_levels(rng, dims, pieces, smallest, top_value):
    def one(position, parts):
        heights = jax.random.uniform(jax.random.fold_in(jax.random.fold_in(rng, 6), position), (parts,), jnp.float32, smallest / len(pieces), top_value / len(pieces))
        return jnp.repeat(jnp.exp(heights), dims[position] // parts).reshape((-1,) + (1,) * (len(dims) - position - 1))

    gain = one(*pieces[0])
    for cut in pieces[1:]:
        gain = gain * one(*cut)
    return gain


def gaussian_with(own_key, shape, scale, most, shards, heavy, kind=jnp.bfloat16):
    values = scale * jax.random.normal(own_key, shape, jnp.float32)
    if shards:
        values = values * block_levels(own_key, shape, shards, -0.22, 0.18)
    return jnp.clip(strengthened(values, jax.random.fold_in(own_key, 3), *heavy), -most, most).astype(kind)


def setup_inputs(seed: int = 0) -> dict:
    seeds = jax.random.split(jax.random.key(seed), 7)
    return {
        "density": gaussian_with(seeds[0], (ENERGIES, KPOINTS, LAYERS, ORBITALS), 1.0, 6.0, ((0, 16), (1, 8)), (0, 2, 16, 2.0)),
        "quad_weights": jnp.clip(jnp.exp(math.log(0.088388346) - 1.3862944 * jax.random.uniform(seeds[1], (ENERGIES, KPOINTS), jnp.float32) ** block_levels(seeds[1], (ENERGIES, KPOINTS), ((0, 16), (1, 8)), -0.2, 0.2)), 0.022097087, 0.088388346),
        "orbital_cells": with_ends(jax.random.randint(seeds[2], (LAYERS, ORBITALS), 0, SUB * NY * NZ), jax.random.fold_in(seeds[2], 1), 0, (SUB * NY * NZ) - 1).astype(jnp.int32),
        "fixed_charge": draw_fixed_charge(jax.random.fold_in(seeds[6], 71), 0),
        "gate_mask": with_ends((jax.random.randint(seeds[4], (GX, NY, NZ), 0, 4) < 1).astype(jnp.int32), jax.random.fold_in(seeds[4], 1), 0, 1),
        "gate_voltage": jnp.clip(jax.random.uniform(seeds[5], (GX,), jnp.float32, -1.0, 1.0) * block_levels(seeds[5], (GX,), ((0, 16),), -0.4, 0.0), -1.0, 1.0),
    }


PENALTY = 4.0


def operate(values_field, diagonal):
    padded = jnp.pad(values_field, 1)
    beside = padded[2:, 1:-1, 1:-1] + padded[:-2, 1:-1, 1:-1]
    beside = beside + padded[1:-1, 2:, 1:-1] + padded[1:-1, :-2, 1:-1]
    beside = beside + padded[1:-1, 1:-1, 2:] + padded[1:-1, 1:-1, :-2]
    return diagonal * values_field - beside


def reference(density, quad_weights, orbital_cells, fixed_charge, gate_mask, gate_voltage):
    occupancy = jnp.einsum("ek,eklo->lo", quad_weights.astype(jnp.float32), density.astype(jnp.float32), precision=lax.Precision.HIGHEST)
    section = SUB * NY * NZ
    layer_base = (jnp.arange(LAYERS, dtype=jnp.int32) * section)[:, None]
    flat_cell = (orbital_cells + layer_base).reshape(-1)
    charge = jax.ops.segment_sum(occupancy.reshape(-1), flat_cell, num_segments=LAYERS * section).reshape(GX, NY, NZ)
    gated = gate_mask.astype(jnp.float32)
    diagonal = 6.0 + PENALTY * gated
    right_side = fixed_charge - charge + PENALTY * gated * gate_voltage[:, None, None]
    potential = jnp.zeros_like(right_side)
    residual = right_side
    direction = right_side
    norm_now = jnp.sum(residual * residual)
    for sweep_index in range(ITERS):
        image = operate(direction, diagonal)
        alpha = norm_now / jnp.sum(direction * image)
        potential = potential + alpha * direction
        residual = residual - alpha * image
        norm_next = jnp.sum(residual * residual)
        direction = residual + (norm_next / norm_now) * direction
        norm_now = norm_next
    orbital_potential = jnp.take_along_axis(potential.reshape(LAYERS, section), orbital_cells, axis=1)
    band_shift = jnp.einsum("eklo,lo->ekl", density.astype(jnp.float32), orbital_potential, precision=lax.Precision.HIGHEST) * (ORBITALS ** -0.5)
    return potential, band_shift
```

```python
import jax
import jax.numpy as jnp
from jax import lax
from jax.experimental import pallas as pl
from jax.experimental.pallas import tpu as pltpu
from jax.sharding import Mesh
from jax.sharding import PartitionSpec as P

ENERGY = ("energy_0", "energy_1")
KPT = ("kpt_0", "kpt_1")
CHIPS = ("energy_0", "energy_1", "kpt_0")
CORE = "kpt_1"
EVERY = ("energy_0", "energy_1", "kpt_0", "kpt_1")

NE = 16
NK = 8
NZC = 4
SUB = 8
LAYERS = 128
LD = 8
ORB = 3072
CY = 16
NY = 128
NZ = 256
PLANES = 64
EL = 4
W = 24
COL = ORB // NK
TL = COL // 128
PENALTY = 4.0
VMEM = 60 * 1024 * 1024


def swap_cores(x):
    return lax.ppermute(x, CORE, [(0, 1), (1, 0)])


def exchange(x, axis):
    return lax.all_to_all(x, axis, split_axis=0, concat_axis=0, tiled=True)


def params():
    return pltpu.CompilerParams(vmem_limit_bytes=VMEM)


def occupancy_body(core, weights, density, own, other):
    for half, out in ((0, own), (1, other)):
        which = core[0] if half == 0 else 1 - core[0]
        start = pl.multiple_of(which * COL, 128)
        zero = jnp.zeros((3, 128), jnp.float32)
        for e in range(0, NE, 2):
            total = None
            for i in range(EL):
                part = density[i, 8 * e : 8 * e + 16, pl.ds(start, COL)].astype(jnp.float32) * weights[i]
                total = part if total is None else total + part
            for h in range(2):
                at = e + h
                for t in range(TL):
                    tile = total[8 * h : 8 * h + 8, 128 * t : 128 * (t + 1)]
                    out[at, 0, 8 * t : 8 * t + 8, :] = tile
                    if at + 1 < NE:
                        out[at + 1, 0, 24 + t : 25 + t, :] = tile[7:8]
                    if at > 0:
                        out[at - 1, 0, 27 + t : 28 + t, :] = tile[0:1]
        out[0, 0, 24:27, :] = zero
        out[NE - 1, 0, 27:30, :] = zero
        for e in range(NE):
            out[e, 0, 30:32, :] = zero[:2]


def occupancy_parts(core, weights, density):
    shape = jax.ShapeDtypeStruct((NE, NZC, 32, 128), jnp.float32)
    block = pl.BlockSpec((NE, 1, 32, 128), lambda z, *_: (0, z, 0, 0))
    return pl.pallas_call(
        occupancy_body,
        grid_spec=pltpu.PrefetchScalarGridSpec(
            num_scalar_prefetch=2,
            grid=(NZC,),
            in_specs=[pl.BlockSpec((EL, LAYERS, 2 * COL), lambda z, *_: (0, 0, z))],
            out_specs=[block, block],
        ),
        out_shape=[shape, shape],
        compiler_params=params(),
        name="occupancy_parts",
    )(core, weights, density)


def collect_body(parts, out):
    total = parts[0]
    for i in range(1, NE * NZC):
        total = total + parts[i]
    for k in range(NK):
        out[k] = total


def collect(parts):
    return pl.pallas_call(
        collect_body,
        out_shape=jax.ShapeDtypeStruct((NK, 32, 128), jnp.float32),
        compiler_params=params(),
        name="collect",
    )(parts)


def split_parts(x):
    high = x.astype(jnp.bfloat16)
    low = (x - high.astype(jnp.float32)).astype(jnp.bfloat16)
    return high, low


def charge_of(cells, values, first_plane, planes, y0):
    count = cells.shape[1]
    plane = (cells >> 15) - first_plane
    dy = ((cells >> 8) & (NY - 1)) - y0
    near = (dy >= -2) & (dy < CY + 2) & (plane >= 0) & (plane < planes)
    row = jnp.where(near, plane * W + jnp.where(dy >= 0, dy, dy + W), -1)
    z = cells & (NZ - 1)
    rows = planes * W
    hit = lax.broadcasted_iota(jnp.int32, (rows, count), 0) == row
    high = values.astype(jnp.bfloat16).astype(jnp.float32)
    low = values - high
    left = jnp.concatenate(
        [jnp.where(hit, high, 0.0).astype(jnp.bfloat16), jnp.where(hit, low, 0.0).astype(jnp.bfloat16)], axis=0
    )
    right = jnp.where(lax.broadcasted_iota(jnp.int32, (NZ, count), 0) == z, 1.0, 0.0).astype(jnp.bfloat16)
    both = lax.dot_general(left, right, (((1,), (1,)), ((), ())), preferred_element_type=jnp.float32)
    return both[:rows] + both[rows:]


def beside(field, plane):
    here = field[plane]
    lane = lax.broadcasted_iota(jnp.int32, (W, NZ), 1)
    total = field[plane + 1] + field[plane - 1]
    total = total + pltpu.roll(here, 1, 0) + pltpu.roll(here, W - 1, 0)
    total = total + jnp.where(lane == 0, 0.0, pltpu.roll(here, 1, 1))
    return here, total + jnp.where(lane == NZ - 1, 0.0, pltpu.roll(here, NZ - 1, 1))


def field_body(where, volts, occ, below, mine, above, fixed, gate, xlow, xhigh, ylow, yhigh,
               sums, r_out, w_out, r_ext, w_ext, g_ext):
    e = where[0]
    k = where[1]
    y0 = k * CY
    row = lax.broadcasted_iota(jnp.int32, (W, NZ), 0)
    y = jnp.where(row < CY + 4, row, row - W) + y0
    valid = jnp.where((y >= 0) & (y < NY), 1.0, 0.0)
    r_ext[:, 16:24, :] = jnp.zeros((PLANES + 4, 8, NZ), jnp.float32)
    g_ext[:, 16:24, :] = jnp.zeros((PLANES + 4, 8, NZ), jnp.float32)

    def load_plane(p, carry):
        g = gate[p].astype(jnp.float32)
        g_ext[p + 2, 0:CY, :] = g
        r_ext[p + 2, 0:CY, :] = fixed[p] + PENALTY * g * volts[p]
        return carry

    lax.fori_loop(0, PLANES, load_plane, 0, unroll=4)
    for i in range(2):
        r_ext[i, 0:CY, :] = xlow[0, i]
        g_ext[i, 0:CY, :] = xlow[1, i]
        r_ext[PLANES + 2 + i, 0:CY, :] = xhigh[0, i]
        g_ext[PLANES + 2 + i, 0:CY, :] = xhigh[1, i]

    def load_halo(p, carry):
        r_ext[p, CY : CY + 2, :] = yhigh[0, p]
        g_ext[p, CY : CY + 2, :] = yhigh[1, p]
        r_ext[p, W - 2 : W, :] = ylow[0, p]
        g_ext[p, W - 2 : W, :] = ylow[1, p]
        return carry

    lax.fori_loop(0, PLANES + 4, load_halo, 0, unroll=4)

    def values_of(index):
        return jnp.concatenate(
            [occ[c, pl.ds(index(t), 1), :] for c in range(NK) for t in range(TL)], axis=1
        )

    def one_layer(j, carry):
        charge = charge_of(mine[pl.ds(j, 1), :], values_of(lambda t: 8 * t + j), 0, SUB, y0)
        at = pl.ds(2 + SUB * j, SUB)
        r_ext[at] = r_ext[at] - charge.reshape(SUB, W, NZ)
        return carry

    lax.fori_loop(0, LD, one_layer, 0)
    charge = charge_of(below[7:8, :], values_of(lambda t: 24 + t), SUB - 2, 2, y0)
    r_ext[0:2] = r_ext[0:2] - charge.reshape(2, W, NZ)
    charge = charge_of(above[0:1, :], values_of(lambda t: 27 + t), 0, 2, y0)
    r_ext[PLANES + 2 : PLANES + 4] = r_ext[PLANES + 2 : PLANES + 4] - charge.reshape(2, W, NZ)

    def image_plane(p, carry):
        here, around = beside(r_ext, p + 1)
        x = e * PLANES + p - 1
        inside = jnp.where((x >= 0) & (x < NE * PLANES), 1.0, 0.0)
        w_ext[p] = ((6.0 + PENALTY * g_ext[p + 1]) * here - around) * (valid * inside)
        return carry

    lax.fori_loop(0, PLANES + 2, image_plane, 0, unroll=2)

    def sum_plane(p, carry):
        rr, rw, ww, waw = carry
        r = r_ext[p + 2, 0:CY, :]
        here, around = beside(w_ext, p + 1)
        image = (6.0 + PENALTY * g_ext[p + 2]) * here - around
        w = here[0:CY]
        r_out[p] = r
        w_out[p] = w
        return rr + r * r, rw + r * w, ww + w * w, waw + w * image[0:CY]

    zero = jnp.zeros((CY, NZ), jnp.float32)
    totals = lax.fori_loop(0, PLANES, sum_plane, (zero,) * 4, unroll=2)
    lane = lax.broadcasted_iota(jnp.int32, (1, 128), 1)
    line = jnp.zeros((1, 128), jnp.float32)
    for i, total in enumerate(totals):
        line = line + jnp.where(lane == i, jnp.sum(total), 0.0)
    for d in range(NE * NK):
        sums[d] = line


def fields(where, volts, occ, cells, fixed, gate, xlow, xhigh, ylow, yhigh):
    whole = lambda x: pl.BlockSpec(x.shape, lambda i, *_: (0,) * x.ndim)
    near = lambda shift: pl.BlockSpec(
        (LD, ORB), lambda i, where, *_: (jnp.clip(where[0] + shift, 0, NE - 1), 0)
    )
    shapes = [
        jax.ShapeDtypeStruct((NE * NK, 1, 128), jnp.float32),
        jax.ShapeDtypeStruct((PLANES, CY, NZ), jnp.float32),
        jax.ShapeDtypeStruct((PLANES, CY, NZ), jnp.float32),
    ]
    return pl.pallas_call(
        field_body,
        grid_spec=pltpu.PrefetchScalarGridSpec(
            num_scalar_prefetch=2,
            grid=(1,),
            in_specs=[whole(occ), near(-1), near(0), near(1)]
            + [whole(x) for x in (fixed, gate, xlow, xhigh, ylow, yhigh)],
            out_specs=[whole(x) for x in shapes],
            scratch_shapes=[
                pltpu.VMEM((PLANES + 4, W, NZ), jnp.float32),
                pltpu.VMEM((PLANES + 2, W, NZ), jnp.float32),
                pltpu.VMEM((PLANES + 4, W, NZ), jnp.float32),
            ],
        ),
        out_shape=shapes,
        compiler_params=params(),
        name="fields",
    )(where, volts, occ, cells, cells, cells, fixed, gate, xlow, xhigh, ylow, yhigh)


def pick_body(where, mine, r, w, out):
    y0 = where[1] * CY
    wide = 2 * COL

    def one_layer(j, carry):
        at = pl.ds(SUB * j, SUB)
        both = jnp.concatenate([r[at].reshape(SUB * CY, NZ), w[at].reshape(SUB * CY, NZ)], axis=0)
        high, low = split_parts(both)
        for n in range(ORB // wide):
            cells = mine[pl.ds(j, 1), n * wide : (n + 1) * wide]
            dy = ((cells >> 8) & (NY - 1)) - y0
            row = jnp.where((dy >= 0) & (dy < CY), (cells >> 15) * CY + dy, -1)
            z = cells & (NZ - 1)
            right = jnp.where(lax.broadcasted_iota(jnp.int32, (NZ, wide), 0) == z, 1.0, 0.0).astype(jnp.bfloat16)
            lines = jnp.dot(high, right, preferred_element_type=jnp.float32)
            lines = lines + jnp.dot(low, right, preferred_element_type=jnp.float32)
            hit = lax.broadcasted_iota(jnp.int32, (SUB * CY, wide), 0) == row
            for f in range(2):
                part = lines[f * SUB * CY : (f + 1) * SUB * CY]
                value = jnp.sum(jnp.where(hit, part, 0.0), axis=0, keepdims=True)
                for h in range(2):
                    out[2 * n + h, pl.ds(f * LD + j, 1), :] = value[:, h * COL : (h + 1) * COL]
        return carry

    lax.fori_loop(0, LD, one_layer, 0)


def pick(where, cells, r, w):
    whole = lambda x: pl.BlockSpec(x.shape, lambda i, *_: (0,) * x.ndim)
    shape = jax.ShapeDtypeStruct((NK, 2 * LD, COL), jnp.float32)
    return pl.pallas_call(
        pick_body,
        grid_spec=pltpu.PrefetchScalarGridSpec(
            num_scalar_prefetch=1,
            grid=(1,),
            in_specs=[pl.BlockSpec((LD, ORB), lambda i, where: (where[0], 0)), whole(r), whole(w)],
            out_specs=whole(shape),
        ),
        out_shape=shape,
        compiler_params=params(),
        name="pick",
    )(where, cells, r, w)


def mix_body(sums, picked, scalars, out):
    line = jnp.sum(sums[...].reshape(NE * NK, 128), axis=0, keepdims=True)
    lane = lax.broadcasted_iota(jnp.int32, (1, 128), 1)
    rr, rw, ww, waw = [
        jnp.broadcast_to(jnp.sum(jnp.where(lane == i, line, 0.0), axis=1, keepdims=True), (1, 128)) for i in range(4)
    ]
    alpha = rr / rw
    norm = alpha * alpha * ww - rr
    ratio = norm / rr
    ahead = 1.0 + ratio
    curve = ahead * ahead * rw - 2.0 * ahead * alpha * ww + alpha * alpha * waw
    small = (norm <= 1e-9 * rr) | (curve <= 0.0)
    step = jnp.where(small, alpha, norm / curve)
    ahead = jnp.where(small, 1.0, ahead)
    c_r = alpha + step * ahead
    c_w = -alpha * step
    scalars[...] = jnp.where(lane == 0, c_r, c_w)
    total = picked[0]
    for i in range(1, NK):
        total = total + picked[i]
    c_r = jnp.concatenate([c_r] * TL, axis=1)
    c_w = jnp.concatenate([c_w] * TL, axis=1)
    value = c_r * total[:LD] + c_w * total[LD:]
    for d in range(NE * NZC):
        out[d] = value


def mix(sums, picked):
    return pl.pallas_call(
        mix_body,
        out_shape=[
            jax.ShapeDtypeStruct((1, 128), jnp.float32),
            jax.ShapeDtypeStruct((NE * NZC, LD, COL), jnp.float32),
        ],
        compiler_params=params(),
        name="mix",
    )(sums, picked)


def band_body(core, density, same, cross, out, acc):
    z = pl.program_id(0)

    @pl.when(z == 0)
    def _():
        acc[...] = jnp.zeros_like(acc)

    for half, values in ((0, same), (1, cross)):
        which = core[0] if half == 0 else 1 - core[0]
        start = pl.multiple_of(which * COL, 128)
        for m in range(0, NE, 2):
            v = values[m : m + 2, 0].reshape(16, COL)
            for i in range(EL):
                part = density[i, 8 * m : 8 * m + 16, pl.ds(start, COL)].astype(jnp.float32) * v
                total = part[:, :128]
                for t in range(1, TL):
                    total = total + part[:, 128 * t : 128 * (t + 1)]
                acc[i, 8 * m : 8 * m + 16] = acc[i, 8 * m : 8 * m + 16] + total

    @pl.when(z == NZC - 1)
    def _():
        for i in range(EL):
            out[i : i + 1, :] = jnp.sum(acc[i].T, axis=0, keepdims=True) * ORB**-0.5


def band(core, density, same, cross):
    values = pl.BlockSpec((NE, 1, LD, COL), lambda z, *_: (0, z, 0, 0))
    return pl.pallas_call(
        band_body,
        grid_spec=pltpu.PrefetchScalarGridSpec(
            num_scalar_prefetch=1,
            grid=(NZC,),
            in_specs=[pl.BlockSpec((EL, LAYERS, 2 * COL), lambda z, *_: (0, 0, z)), values, values],
            out_specs=pl.BlockSpec((EL, LAYERS), lambda z, *_: (0, 0)),
            scratch_shapes=[pltpu.VMEM((EL, LAYERS, 128), jnp.float32)],
        ),
        out_shape=jax.ShapeDtypeStruct((EL, LAYERS), jnp.float32),
        compiler_params=params(),
        name="band",
    )(core, density, same, cross)


def edges(x, axis, dim):
    peers = lax.axis_size(axis)
    up = [(i, i + 1) for i in range(peers - 1)]
    first = lax.slice_in_dim(x, 0, 2, axis=dim)
    last = lax.slice_in_dim(x, x.shape[dim] - 2, x.shape[dim], axis=dim)
    return lax.ppermute(last, axis, up), lax.ppermute(first, axis, [(b, a) for a, b in up])


def per_device(density, quad_weights, orbital_cells, fixed_charge, gate_mask, gate_voltage):
    e = lax.axis_index(ENERGY).astype(jnp.int32)
    k = lax.axis_index(KPT).astype(jnp.int32)
    core = lax.axis_index(CORE).astype(jnp.int32)[None]
    where = jnp.stack([e, k])
    density = density.reshape(EL, LAYERS, ORB)

    own, other = occupancy_parts(core, quad_weights.reshape(EL), density)
    chips = NE * NZC
    pair = own.reshape(chips, 32, 128) + swap_cores(other.reshape(chips, 32, 128))
    parts = exchange(pair, CHIPS)

    gated = gate_mask.astype(jnp.float32)
    known = jnp.stack([fixed_charge + PENALTY * gated * gate_voltage[:, None, None], gated])
    xlow, xhigh = edges(known, ENERGY, 1)
    first = jnp.concatenate([xlow[:, :, :2], known[:, :, :2], xhigh[:, :, :2]], axis=1)
    last = jnp.concatenate([xlow[:, :, -2:], known[:, :, -2:], xhigh[:, :, -2:]], axis=1)
    up = [(i, i + 1) for i in range(NK - 1)]
    ylow = lax.ppermute(last, KPT, up)
    yhigh = lax.ppermute(first, KPT, [(b, a) for a, b in up])

    occ = exchange(collect(parts), KPT)
    sums, r, w = fields(
        where, gate_voltage, occ, orbital_cells, fixed_charge, gate_mask, xlow, xhigh, ylow, yhigh
    )
    all_sums = exchange(sums, EVERY)
    picked = exchange(pick(where, orbital_cells, r, w), KPT)
    scalars, values = mix(all_sums, picked)
    same = exchange(values, CHIPS)
    potential = scalars[0, 0] * r + scalars[0, 1] * w
    cross = swap_cores(same)
    shape = (NE, NZC, LD, COL)
    shift = band(core, density, same.reshape(shape), cross.reshape(shape))
    return potential, shift.reshape(EL, 1, LAYERS)


def solution(mesh):
    split = Mesh(mesh.devices.reshape(4, 4, 4, 2), ("energy_0", "energy_1", "kpt_0", "kpt_1"))
    in_specs = (
        P(ENERGY, KPT, None, None),
        P(ENERGY, KPT),
        P(),
        P(ENERGY, KPT, None),
        P(ENERGY, KPT, None),
        P(ENERGY),
    )
    out_specs = (P(ENERGY, KPT, None), P(ENERGY, KPT, None))
    return jax.shard_map(per_device, mesh=split, in_specs=in_specs, out_specs=out_specs, check_vma=False)
```

```python
import jax
import jax.numpy as jnp
from jax import lax
from jax.experimental import pallas as pl
from jax.experimental.pallas import tpu as pltpu
from jax.sharding import Mesh
from jax.sharding import PartitionSpec as P

ENERGY = ("energy_0", "energy_1")
KPT = ("kpt_0", "kpt_1")
CHIPS = ("energy_0", "energy_1", "kpt_0")
CORE = "kpt_1"
EVERY = ("energy_0", "energy_1", "kpt_0", "kpt_1")

NE = 16
NK = 8
NZC = 4
SUB = 8
LAYERS = 128
LD = 8
ORB = 3072
CY = 16
NY = 128
NZ = 256
PLANES = 64
EL = 4
W = 24
COL = ORB // NK
TL = COL // 128
PENALTY = 4.0


def swap_cores(x):
    return lax.ppermute(x, CORE, [(0, 1), (1, 0)])


def exchange(x, axis):
    return lax.all_to_all(x, axis, split_axis=0, concat_axis=0, tiled=True)


def in_hbm(x):
    return pltpu.with_memory_space_constraint(x, pltpu.HBM)


def params(mib):
    return pltpu.CompilerParams(vmem_limit_bytes=mib * 1024 * 1024)


def occupancy_body(energy, kpt, volts, weights, density, fixed, gate, own, other, xup, xdown, yup, ydown,
                   fixed_here, gate_here, fixed_ends, gate_ends, arrivals):
    z = pl.program_id(0)
    e = energy[0]
    k = kpt[0]
    core = k % 2
    whole = [
        pltpu.make_async_copy(fixed, fixed_here, arrivals.at[0]),
        pltpu.make_async_copy(gate, gate_here, arrivals.at[1]),
    ]
    ends = []
    for i, plane in enumerate((0, PLANES - 1)):
        ends.append(pltpu.make_async_copy(fixed.at[plane], fixed_ends.at[i], arrivals.at[2 + 2 * i]))
        ends.append(pltpu.make_async_copy(gate.at[plane], gate_ends.at[i], arrivals.at[3 + 2 * i]))

    @pl.when(z == 0)
    def _():
        for copy in ends + whole:
            copy.start()

    for half, out in ((0, own), (1, other)):
        which = core if half == 0 else 1 - core
        start = pl.multiple_of(which * COL, 128)
        zero = jnp.zeros((3, 128), jnp.float32)
        for i in range(0, NE, 2):
            total = None
            for n in range(EL):
                weight = jnp.broadcast_to(weights[0:1, n : n + 1], (16, COL))
                part = density[n, 8 * i : 8 * i + 16, pl.ds(start, COL)].astype(jnp.float32) * weight
                total = part if total is None else total + part
            for h in range(2):
                at = i + h
                for t in range(TL):
                    tile = total[8 * h : 8 * h + 8, 128 * t : 128 * (t + 1)]
                    out[at, 0, 8 * t : 8 * t + 8, :] = tile
                    if at + 1 < NE:
                        out[at + 1, 0, 24 + t : 25 + t, :] = tile[7:8]
                    if at > 0:
                        out[at - 1, 0, 27 + t : 28 + t, :] = tile[0:1]
        out[0, 0, 24:27, :] = zero
        out[NE - 1, 0, 27:30, :] = zero
        for i in range(NE):
            out[i, 0, 30:32, :] = zero[:2]

    @pl.when(z == 0)
    def _():
        for copy in ends:
            copy.wait()

    for dx in (-1, 1):
        for dy in (-1, 1):
            to_e = e + dx
            to_k = k + dy

            @pl.when((to_e >= 0) & (to_e < NE) & (to_k >= 0) & (to_k < NK) & (to_k // 2 == z))
            def _(dx=dx, dy=dy, to_e=to_e):
                i = 1 if dx == 1 else 0
                y = CY - 1 if dy == 1 else 0
                g = gate_ends[i, y : y + 1, :].astype(jnp.float32)
                line = fixed_ends[i, y : y + 1, :] + PENALTY * g * volts[(PLANES - 1) * i]
                other[to_e, 0, 30:31, :] = line[:, :128]
                other[to_e, 0, 31:32, :] = line[:, 128:]

    @pl.when(z == NZC - 1)
    def _():
        for copy in whole:
            copy.wait()
        for out, planes in ((xup, (PLANES - 2, PLANES - 1)), (xdown, (0, 1))):
            for i, p in enumerate(planes):
                g = gate_here[p].astype(jnp.float32)
                out[i] = fixed_here[p] + PENALTY * g * volts[p]
                if p in (0, PLANES - 1):
                    out[2] = g

        def one_plane(p, carry):
            volt = PENALTY * volts[p]
            for out, rows in ((yup, (CY - 2, CY - 1)), (ydown, (0, 1))):
                for i, y in enumerate(rows):
                    g = gate_here[p, y : y + 1, :].astype(jnp.float32)
                    out[i, pl.ds(p, 1), :] = fixed_here[p, y : y + 1, :] + volt * g
                    if y in (0, CY - 1):
                        out[2, pl.ds(p, 1), :] = g
            return carry

        lax.fori_loop(0, PLANES, one_plane, 0, unroll=8)


def occupancy_parts(e, k, volts, weights, density, fixed, gate):
    shape = jax.ShapeDtypeStruct((NE, NZC, 32, 128), jnp.float32)
    block = pl.BlockSpec((NE, 1, 32, 128), lambda z, *_: (0, z, 0, 0))
    xedge = jax.ShapeDtypeStruct((3, CY, NZ), jnp.float32)
    yedge = jax.ShapeDtypeStruct((3, PLANES, NZ), jnp.float32)
    whole = lambda x: pl.BlockSpec(x.shape, lambda z, *_: (0, 0, 0))
    hbm = pl.BlockSpec(memory_space=pltpu.HBM)
    return pl.pallas_call(
        occupancy_body,
        grid_spec=pltpu.PrefetchScalarGridSpec(
            num_scalar_prefetch=3,
            grid=(NZC,),
            in_specs=[
                pl.BlockSpec((1, EL), lambda z, *_: (0, 0)),
                pl.BlockSpec((EL, LAYERS, 2 * COL), lambda z, *_: (0, 0, z)),
                hbm,
                hbm,
            ],
            out_specs=[block, block, whole(xedge), whole(xedge), whole(yedge), whole(yedge)],
            scratch_shapes=[
                pltpu.VMEM((PLANES, CY, NZ), jnp.float32),
                pltpu.VMEM((PLANES, CY, NZ), jnp.int32),
                pltpu.VMEM((2, CY, NZ), jnp.float32),
                pltpu.VMEM((2, CY, NZ), jnp.int32),
                pltpu.SemaphoreType.DMA((6,)),
            ],
        ),
        out_shape=[shape, shape, xedge, xedge, yedge, yedge],
        compiler_params=params(12),
        name="occupancy_parts",
    )(e[None], k[None], in_hbm(volts), in_hbm(weights), in_hbm(density), in_hbm(fixed), in_hbm(gate))


def collect_body(where, parts, out, corners):
    e = where[0]
    k = where[1]
    total = parts[0]
    for i in range(1, NE * NZC):
        total = total + parts[i]
    for n in range(NK):
        out[n] = total
    for i, dx in enumerate((-1, 1)):
        for j, dy in enumerate((-1, 1)):
            from_e = e + dx
            from_k = k + dy
            there = (from_e >= 0) & (from_e < NE) & (from_k >= 0) & (from_k < NK)
            source = jnp.where(there, from_e * NZC + from_k // 2, 0)
            lines = parts[source, 30:32, :]
            corners[i, j : j + 1, 0:128] = jnp.where(there, lines[0:1], 0.0)
            corners[i, j : j + 1, 128:256] = jnp.where(there, lines[1:2], 0.0)


def collect(where, parts):
    whole = lambda shape: pl.BlockSpec(shape, lambda i, *_: (0, 0, 0))
    shapes = [(NK, 32, 128), (2, 2, NZ)]
    return pl.pallas_call(
        collect_body,
        grid_spec=pltpu.PrefetchScalarGridSpec(
            num_scalar_prefetch=1,
            grid=(1,),
            in_specs=[whole((NE * NZC, 32, 128))],
            out_specs=[whole(x) for x in shapes],
        ),
        out_shape=[jax.ShapeDtypeStruct(x, jnp.float32) for x in shapes],
        compiler_params=params(4),
        name="collect",
    )(where, parts)


def split_parts(x):
    high = x.astype(jnp.bfloat16)
    low = (x - high.astype(jnp.float32)).astype(jnp.bfloat16)
    return high, low


def spread(line, rows):
    block = jnp.broadcast_to(line, (16, 128)).astype(jnp.bfloat16)
    return jnp.concatenate([block] * (rows // 16), axis=0)


def counting(rows):
    return lax.broadcasted_iota(jnp.int32, (rows, 128), 0).astype(jnp.float32).astype(jnp.bfloat16)


def tiles_of(line):
    return [line[:, 128 * t : 128 * (t + 1)] for t in range(line.shape[1] // 128)]


def marks(index, rows, counts):
    one = jnp.ones((), jnp.bfloat16)
    zero = jnp.zeros((), jnp.bfloat16)
    return jnp.concatenate([jnp.where(counts[:rows] == spread(t, rows), one, zero) for t in tiles_of(index)], axis=1)


def charge_of(cells, values, first_plane, planes, y0):
    plane = (cells >> 15) - first_plane
    dy = ((cells >> 8) & (NY - 1)) - y0
    near = (dy >= -2) & (dy < CY + 2) & (plane >= 0) & (plane < planes)
    row = jnp.where(near, plane * W + jnp.where(dy >= 0, dy, dy + W), -1).astype(jnp.float32)
    z = (cells & (NZ - 1)).astype(jnp.float32)
    rows = planes * W
    counts = counting(NZ)
    high = values.astype(jnp.bfloat16).astype(jnp.float32)
    low = values - high
    zero = jnp.zeros((), jnp.bfloat16)
    tops, bottoms = [], []
    for t, h, l in zip(tiles_of(row), tiles_of(high), tiles_of(low)):
        hit = counts[:rows] == spread(t, rows)
        tops.append(jnp.where(hit, spread(h, rows), zero))
        bottoms.append(jnp.where(hit, spread(l, rows), zero))
    left = jnp.concatenate([jnp.concatenate(tops, axis=1), jnp.concatenate(bottoms, axis=1)], axis=0)
    right = marks(z, NZ, counts)
    both = lax.dot_general(left, right, (((1,), (1,)), ((), ())), preferred_element_type=jnp.float32)
    return both[:rows] + both[rows:]


def beside(field, plane):
    here = field[plane]
    lane = lax.broadcasted_iota(jnp.int32, (W, NZ), 1)
    total = field[plane + 1] + field[plane - 1]
    total = total + pltpu.roll(here, 1, 0) + pltpu.roll(here, W - 1, 0)
    total = total + jnp.where(lane == 0, 0.0, pltpu.roll(here, 1, 1))
    return here, total + jnp.where(lane == NZ - 1, 0.0, pltpu.roll(here, NZ - 1, 1))


def field_body(where, volts, occ, below, mine, above, corners, xlow, xhigh, ylow, yhigh, fixed, gate,
               sums, kept_out, fields_here, r_ext, w_ext, g_ext, fixed_here, gate_here, arrivals, leaving):
    e = where[0]
    k = where[1]
    y0 = k * CY
    copies = [
        pltpu.make_async_copy(fixed, fixed_here, arrivals.at[0]),
        pltpu.make_async_copy(gate, gate_here, arrivals.at[1]),
    ]
    for copy in copies:
        copy.start()
    row = lax.broadcasted_iota(jnp.int32, (W, NZ), 0)
    y = jnp.where(row < CY + 4, row, row - W) + y0
    valid = jnp.where((y >= 0) & (y < NY), 1.0, 0.0)

    def values_of(index):
        return jnp.concatenate(
            [occ[c, pl.ds(index(t), 1), :] for c in range(NK) for t in range(TL)], axis=1
        )

    def one_layer(j, carry):
        charge = charge_of(mine[pl.ds(j, 1), :], values_of(lambda t: 8 * t + j), 0, SUB, y0)
        r_ext[pl.ds(2 + SUB * j, SUB)] = -charge.reshape(SUB, W, NZ)
        return carry

    lax.fori_loop(0, LD, one_layer, 0, unroll=LD)
    charge = charge_of(below[7:8, :], values_of(lambda t: 24 + t), SUB - 2, 2, y0)
    r_ext[0:2] = -charge.reshape(2, W, NZ)
    charge = charge_of(above[0:1, :], values_of(lambda t: 27 + t), 0, 2, y0)
    r_ext[PLANES + 2 : PLANES + 4] = -charge.reshape(2, W, NZ)

    for at, halo in ((0, xlow), (PLANES + 2, xhigh)):
        for i in range(2):
            r_ext[at + i, 0:CY, :] = r_ext[at + i, 0:CY, :] + halo[i]
    g_ext[1, 0:CY, :] = xlow[2]
    g_ext[PLANES + 2, 0:CY, :] = xhigh[2]
    sub = lax.broadcasted_iota(jnp.int32, (8, NZ), 0)
    none = jnp.zeros((8, NZ), jnp.float32)
    line = lambda x: jnp.broadcast_to(x, (8, NZ))
    for at, i in ((1, 0), (PLANES + 2, 1)):
        tile = jnp.where(sub == 0, line(corners[i, 1:2, :]), jnp.where(sub == 7, line(corners[i, 0:1, :]), none))
        r_ext[at, CY:W, :] = r_ext[at, CY:W, :] + tile
        g_ext[at, CY:W, :] = none
    for copy in copies:
        copy.wait()

    def load_plane(p, carry):
        at = pl.ds(p, 1)
        g = gate_here[p].astype(jnp.float32)
        g_ext[p + 2, 0:CY, :] = g
        r_ext[p + 2, 0:CY, :] = r_ext[p + 2, 0:CY, :] + (fixed_here[p] + PENALTY * g * volts[p])
        tile = jnp.where(sub == 0, line(yhigh[0, at, :]), jnp.where(sub == 1, line(yhigh[1, at, :]), none))
        tile = jnp.where(sub == 6, line(ylow[0, at, :]), jnp.where(sub == 7, line(ylow[1, at, :]), tile))
        r_ext[p + 2, CY:W, :] = r_ext[p + 2, CY:W, :] + tile
        tile = jnp.where(sub == 0, line(yhigh[2, at, :]), jnp.where(sub == 7, line(ylow[2, at, :]), none))
        g_ext[p + 2, CY:W, :] = tile
        return carry

    lax.fori_loop(0, PLANES, load_plane, 0, unroll=8)

    def image_plane(p, carry):
        here, around = beside(r_ext, p + 1)
        x = e * PLANES + p - 1
        inside = jnp.where((x >= 0) & (x < NE * PLANES), 1.0, 0.0)
        w_ext[p] = ((6.0 + PENALTY * g_ext[p + 1]) * here - around) * (valid * inside)
        return carry

    lax.fori_loop(0, PLANES + 2, image_plane, 0, unroll=11)

    def sum_plane(p, carry):
        rr, rw, ww, waw = carry
        r = r_ext[p + 2, 0:CY, :]
        here, around = beside(w_ext, p + 1)
        image = (6.0 + PENALTY * g_ext[p + 2]) * here - around
        w = here[0:CY]
        fields_here[0, p] = r
        fields_here[1, p] = w
        return rr + r * r, rw + r * w, ww + w * w, waw + w * image[0:CY]

    zero = jnp.zeros((CY, NZ), jnp.float32)
    totals = (zero,) * 4
    kept = []
    for j in range(LD):
        totals = lax.fori_loop(SUB * j, SUB * (j + 1), sum_plane, totals, unroll=SUB)
        at = pl.ds(SUB * j, SUB)
        kept.append(pltpu.make_async_copy(fields_here.at[:, at], kept_out.at[:, at], leaving.at[j]))
        kept[-1].start()
    lane = lax.broadcasted_iota(jnp.int32, (1, 128), 1)
    line = jnp.zeros((1, 128), jnp.float32)
    for i, total in enumerate(totals):
        line = line + jnp.where(lane == i, jnp.sum(total), 0.0)
    for d in range(NE * NK):
        sums[d] = line
    for copy in kept:
        copy.wait()


def fields(where, volts, occ, cells, corners, fixed, gate, xlow, xhigh, ylow, yhigh):
    whole = lambda x: pl.BlockSpec(x.shape, lambda i, *_: (0,) * x.ndim)
    near = lambda shift: pl.BlockSpec(
        (LD, ORB), lambda i, where, *_: (jnp.clip(where[0] + shift, 0, NE - 1), 0)
    )
    shapes = [
        jax.ShapeDtypeStruct((NE * NK, 1, 128), jnp.float32),
        pltpu.HBM((2, PLANES, CY, NZ), jnp.float32),
    ]
    return pl.pallas_call(
        field_body,
        grid_spec=pltpu.PrefetchScalarGridSpec(
            num_scalar_prefetch=2,
            grid=(1,),
            in_specs=[whole(occ), near(-1), near(0), near(1)]
            + [whole(x) for x in (corners, xlow, xhigh, ylow, yhigh)]
            + [pl.BlockSpec(memory_space=pltpu.HBM)] * 2,
            out_specs=[
                pl.BlockSpec((NE * NK, 1, 128), lambda i, *_: (0, 0, 0)),
                pl.BlockSpec(memory_space=pltpu.HBM),
            ],
            scratch_shapes=[
                pltpu.VMEM((2, PLANES, CY, NZ), jnp.float32),
                pltpu.VMEM((PLANES + 4, W, NZ), jnp.float32),
                pltpu.VMEM((PLANES + 2, W, NZ), jnp.float32),
                pltpu.VMEM((PLANES + 4, W, NZ), jnp.float32),
                pltpu.VMEM((PLANES, CY, NZ), jnp.float32),
                pltpu.VMEM((PLANES, CY, NZ), jnp.int32),
                pltpu.SemaphoreType.DMA((2,)),
                pltpu.SemaphoreType.DMA((LD,)),
            ],
        ),
        out_shape=shapes,
        compiler_params=params(16),
        name="fields",
    )(where, volts, occ, cells, cells, cells, corners, xlow, xhigh, ylow, yhigh, in_hbm(fixed), in_hbm(gate))


def pick_body(where, mine, rw_kept, out, rw, arrivals):
    copies = []
    for j in range(LD):
        at = pl.ds(SUB * j, SUB)
        copies.append(pltpu.make_async_copy(rw_kept.at[:, at], rw.at[:, at], arrivals.at[j]))
        copies[-1].start()
    y0 = where[1] * CY
    wide = 2 * COL
    counts = counting(NZ)

    def one_layer(j, carry):
        at = pl.ds(SUB * j, SUB)
        both = jnp.concatenate([rw[0, at].reshape(SUB * CY, NZ), rw[1, at].reshape(SUB * CY, NZ)], axis=0)
        high, low = split_parts(both)
        for n in range(ORB // wide):
            cells = mine[pl.ds(j, 1), n * wide : (n + 1) * wide]
            dy = ((cells >> 8) & (NY - 1)) - y0
            row = jnp.where((dy >= 0) & (dy < CY), (cells >> 15) * CY + dy, -1)
            z = cells & (NZ - 1)
            right = marks(z.astype(jnp.float32), NZ, counts)
            lines = jnp.dot(high, right, preferred_element_type=jnp.float32)
            lines = lines + jnp.dot(low, right, preferred_element_type=jnp.float32)
            hit = lax.broadcasted_iota(jnp.int32, (SUB * CY, wide), 0) == row
            for f in range(2):
                part = lines[f * SUB * CY : (f + 1) * SUB * CY]
                value = jnp.sum(jnp.where(hit, part, 0.0), axis=0, keepdims=True)
                for h in range(2):
                    out[2 * n + h, pl.ds(f * LD + j, 1), :] = value[:, h * COL : (h + 1) * COL]
        return carry

    for j in range(LD):
        copies[j].wait()
        one_layer(j, 0)


def pick(where, cells, rw):
    whole = lambda x: pl.BlockSpec(x.shape, lambda i, *_: (0,) * x.ndim)
    shape = jax.ShapeDtypeStruct((NK, 2 * LD, COL), jnp.float32)
    return pl.pallas_call(
        pick_body,
        grid_spec=pltpu.PrefetchScalarGridSpec(
            num_scalar_prefetch=1,
            grid=(1,),
            in_specs=[pl.BlockSpec((LD, ORB), lambda i, where: (where[0], 0)), pl.BlockSpec(memory_space=pltpu.HBM)],
            out_specs=whole(shape),
            scratch_shapes=[pltpu.VMEM(rw.shape, jnp.float32), pltpu.SemaphoreType.DMA((LD,))],
        ),
        out_shape=shape,
        compiler_params=params(12),
        name="pick",
    )(where, cells, in_hbm(rw))


def mix_body(sums, picked, scalars, out):
    line = jnp.sum(sums[...].reshape(NE * NK, 128), axis=0, keepdims=True)
    lane = lax.broadcasted_iota(jnp.int32, (1, 128), 1)
    rr, rw, ww, waw = [
        jnp.broadcast_to(jnp.sum(jnp.where(lane == i, line, 0.0), axis=1, keepdims=True), (1, 128)) for i in range(4)
    ]
    alpha = rr / rw
    norm = alpha * alpha * ww - rr
    ratio = norm / rr
    ahead = 1.0 + ratio
    curve = ahead * ahead * rw - 2.0 * ahead * alpha * ww + alpha * alpha * waw
    small = (norm <= 1e-9 * rr) | (curve <= 0.0)
    step = jnp.where(small, alpha, norm / curve)
    ahead = jnp.where(small, 1.0, ahead)
    c_r = alpha + step * ahead
    c_w = -alpha * step
    scalars[...] = jnp.where(lane == 0, c_r, c_w)
    total = picked[0]
    for i in range(1, NK):
        total = total + picked[i]
    c_r = jnp.concatenate([c_r] * TL, axis=1)
    c_w = jnp.concatenate([c_w] * TL, axis=1)
    value = c_r * total[:LD] + c_w * total[LD:]
    for d in range(NE * NZC):
        out[d] = value


def mix(sums, picked):
    return pl.pallas_call(
        mix_body,
        out_shape=[
            jax.ShapeDtypeStruct((1, 128), jnp.float32),
            pltpu.HBM((NE * NZC, LD, COL), jnp.float32),
        ],
        compiler_params=params(4),
        name="mix",
    )(sums, picked)


def blend_body(scalars, rw, out):
    c_r = jnp.broadcast_to(scalars[0:1, 0:1], (CY, NZ))
    c_w = jnp.broadcast_to(scalars[0:1, 1:2], (CY, NZ))

    def one_plane(p, carry):
        out[p] = c_r * rw[0, p] + c_w * rw[1, p]
        return carry

    lax.fori_loop(0, PLANES, one_plane, 0, unroll=8)


def blend(scalars, rw):
    return pl.pallas_call(
        blend_body,
        out_shape=jax.ShapeDtypeStruct((PLANES, CY, NZ), jnp.float32),
        compiler_params=params(6),
        name="blend",
    )(scalars, rw)


def band_body(core, density, same, cross, out, acc):
    z = pl.program_id(0)

    @pl.when(z == 0)
    def _():
        acc[...] = jnp.zeros_like(acc)

    for half, values in ((0, same), (1, cross)):
        which = core[0] if half == 0 else 1 - core[0]
        start = pl.multiple_of(which * COL, 128)
        for m in range(0, NE, 2):
            v = values[m : m + 2, 0].reshape(16, COL)
            for i in range(EL):
                part = density[i, 8 * m : 8 * m + 16, pl.ds(start, COL)].astype(jnp.float32) * v
                total = part[:, :128]
                for t in range(1, TL):
                    total = total + part[:, 128 * t : 128 * (t + 1)]
                acc[i, 8 * m : 8 * m + 16] = acc[i, 8 * m : 8 * m + 16] + total

    @pl.when(z == NZC - 1)
    def _():
        for i in range(EL):
            out[i : i + 1, :] = jnp.sum(acc[i].T, axis=0, keepdims=True) * ORB**-0.5


def band(core, density, same, cross):
    values = pl.BlockSpec((NE, 1, LD, COL), lambda z, *_: (0, z, 0, 0))
    return pl.pallas_call(
        band_body,
        grid_spec=pltpu.PrefetchScalarGridSpec(
            num_scalar_prefetch=1,
            grid=(NZC,),
            in_specs=[pl.BlockSpec((EL, LAYERS, 2 * COL), lambda z, *_: (0, 0, z)), values, values],
            out_specs=pl.BlockSpec((EL, LAYERS), lambda z, *_: (0, 0)),
            scratch_shapes=[pltpu.VMEM((EL, LAYERS, 128), jnp.float32)],
        ),
        out_shape=jax.ShapeDtypeStruct((EL, LAYERS), jnp.float32),
        compiler_params=params(8),
        name="band",
    )(core, density, same, cross)


def shift_up(x, axis):
    return lax.ppermute(x, axis, [(i, i + 1) for i in range(lax.axis_size(axis) - 1)])


def shift_down(x, axis):
    return lax.ppermute(x, axis, [(i + 1, i) for i in range(lax.axis_size(axis) - 1)])


def one_step(density, quad_weights, orbital_cells, fixed_charge, gate_mask, gate_voltage):
    e = lax.axis_index(ENERGY).astype(jnp.int32)
    k = lax.axis_index(KPT).astype(jnp.int32)
    core = lax.axis_index(CORE).astype(jnp.int32)[None]
    where = jnp.stack([e, k])
    density = density.reshape(EL, LAYERS, ORB)

    own, other, xup, xdown, yup, ydown = occupancy_parts(
        e, k, gate_voltage, quad_weights.reshape(1, EL), density, fixed_charge, gate_mask
    )
    chips = NE * NZC
    pair = own.reshape(chips, 32, 128) + swap_cores(other.reshape(chips, 32, 128))
    parts = exchange(pair, CHIPS)
    xlow = shift_up(xup, ENERGY)
    xhigh = shift_down(xdown, ENERGY)
    ylow = shift_up(yup, KPT)
    yhigh = shift_down(ydown, KPT)
    parts, xlow, xhigh = lax.optimization_barrier((parts, xlow, xhigh))
    occ, corners = collect(where, parts)
    occ = exchange(occ, KPT)
    sums, rw = fields(
        where, gate_voltage, occ, orbital_cells, corners, fixed_charge, gate_mask, xlow, xhigh, ylow, yhigh
    )
    all_sums = exchange(sums, EVERY)
    picked = pick(where, orbital_cells, rw)
    picked = exchange(picked, KPT)
    scalars, values = mix(all_sums, picked)
    same = exchange(values, CHIPS)
    potential = blend(scalars, rw)
    cross = swap_cores(same)
    shape = (NE, NZC, LD, COL)
    shift = band(core, density, same.reshape(shape), cross.reshape(shape))
    return potential, shift.reshape(EL, 1, LAYERS)


def solution(mesh):
    split = Mesh(mesh.devices.reshape(4, 4, 4, 2), ("energy_0", "energy_1", "kpt_0", "kpt_1"))
    in_specs = (
        P(ENERGY, KPT, None, None),
        P(ENERGY, KPT),
        P(),
        P(ENERGY, KPT, None),
        P(ENERGY, KPT, None),
        P(ENERGY),
    )
    out_specs = (P(ENERGY, KPT, None), P(ENERGY, KPT, None))
    return jax.shard_map(one_step, mesh=split, in_specs=in_specs, out_specs=out_specs, check_vma=False)
```

```python
import jax
import jax.numpy as jnp
from jax import lax
from jax.experimental import pallas as pl
from jax.experimental.pallas import tpu as pltpu
from jax.sharding import Mesh
from jax.sharding import PartitionSpec as P

ENERGY = ("energy_0", "energy_1")
KPT = ("kpt_0", "kpt_1")
CHIPS = ("energy_0", "energy_1", "kpt_0")
CORE = "kpt_1"
EVERY = ("energy_0", "energy_1", "kpt_0", "kpt_1")

NE = 16
NK = 8
NZC = 4
SUB = 8
LAYERS = 128
LD = 8
ORB = 3072
CY = 16
NY = 128
NZ = 256
PLANES = 64
EL = 4
W = 24
WC = 20
COL = ORB // NK
TL = COL // 128
PENALTY = 4.0


def swap_cores(x):
    return lax.ppermute(x, CORE, [(0, 1), (1, 0)])


def exchange(x, axis):
    return lax.all_to_all(x, axis, split_axis=0, concat_axis=0, tiled=True)


def in_hbm(x):
    return pltpu.with_memory_space_constraint(x, pltpu.HBM)


def params(mib):
    return pltpu.CompilerParams(vmem_limit_bytes=mib * 1024 * 1024)


def occupancy_body(energy, kpt, weights, density, volts_out, fixed, gate, own, other, fixed_ends, gate_ends, volts, arrivals):
    step = pl.program_id(0)
    e = energy[0]
    k = kpt[0]
    core = k % 2
    z = chip_order(step, kpt)
    ends = [pltpu.make_async_copy(volts_out, volts, arrivals.at[4])]
    for i, plane in enumerate((0, PLANES - 1)):
        ends.append(pltpu.make_async_copy(fixed.at[plane], fixed_ends.at[i], arrivals.at[2 * i]))
        ends.append(pltpu.make_async_copy(gate.at[plane], gate_ends.at[i], arrivals.at[2 * i + 1]))

    @pl.when(step == 0)
    def _():
        for copy in ends:
            copy.start()

    for half, out in ((0, own), (1, other)):
        which = core if half == 0 else 1 - core
        start = pl.multiple_of(which * COL, 128)
        zero = jnp.zeros((3, 128), jnp.float32)
        for i in range(0, NE, 2):
            total = None
            for n in range(EL):
                weight = jnp.broadcast_to(weights[0:1, n : n + 1], (16, COL))
                part = density[n, 8 * i : 8 * i + 16, pl.ds(start, COL)].astype(jnp.float32) * weight
                total = part if total is None else total + part
            for h in range(2):
                at = i + h
                for t in range(TL):
                    tile = total[8 * h : 8 * h + 8, 128 * t : 128 * (t + 1)]
                    out[at, 0, 8 * t : 8 * t + 8, :] = tile
                    if at + 1 < NE:
                        out[at + 1, 0, 24 + t : 25 + t, :] = tile[7:8]
                    if at > 0:
                        out[at - 1, 0, 27 + t : 28 + t, :] = tile[0:1]
        out[0, 0, 24:27, :] = zero
        out[NE - 1, 0, 27:30, :] = zero
        for i in range(NE):
            out[i, 0, 30:32, :] = zero[:2]

    @pl.when(step == 1)
    def _():
        for copy in ends:
            copy.wait()

    for dx in (-1, 1):
        for dy in (-1, 1):
            to_e = e + dx
            to_k = k + dy

            @pl.when((to_e >= 0) & (to_e < NE) & (to_k >= 0) & (to_k < NK) & (to_k // 2 == z))
            def _(dx=dx, dy=dy, to_e=to_e):
                i = 1 if dx == 1 else 0
                y = CY - 1 if dy == 1 else 0
                g = gate_ends[i, y : y + 1, :].astype(jnp.float32)
                line = fixed_ends[i, y : y + 1, :] + PENALTY * g * volts[(PLANES - 1) * i]
                other[to_e, 0, 30:31, :] = line[:, :128]
                other[to_e, 0, 31:32, :] = line[:, 128:]


def chip_order(step, kpt):
    return (kpt[0] // 2 + 2 + step) % NZC


def occupancy_parts(e, k, volts, weights, density, fixed, gate):
    shape = jax.ShapeDtypeStruct((NE, NZC, 32, 128), jnp.float32)
    block = pl.BlockSpec((NE, 1, 32, 128), lambda i, e, k: (0, chip_order(i, k), 0, 0))
    hbm = pl.BlockSpec(memory_space=pltpu.HBM)
    return pl.pallas_call(
        occupancy_body,
        grid_spec=pltpu.PrefetchScalarGridSpec(
            num_scalar_prefetch=2,
            grid=(NZC,),
            in_specs=[
                pl.BlockSpec((1, EL), lambda z, *_: (0, 0)),
                pl.BlockSpec((EL, LAYERS, 2 * COL), lambda i, e, k: (0, 0, chip_order(i, k))),
                hbm,
                hbm,
                hbm,
            ],
            out_specs=[block, block],
            scratch_shapes=[
                pltpu.VMEM((2, CY, NZ), jnp.float32),
                pltpu.VMEM((2, CY, NZ), jnp.int32),
                pltpu.SMEM((PLANES,), jnp.float32),
                pltpu.SemaphoreType.DMA((5,)),
            ],
        ),
        out_shape=[shape, shape],
        compiler_params=params(8),
        name="occupancy_parts",
    )(e[None], k[None], in_hbm(weights), in_hbm(density), in_hbm(volts), in_hbm(fixed), in_hbm(gate))


def edges_body(energy, volts_out, fixed, gate, cells, xup, xdown, yup, ydown, near, fixed_here, gate_here, volts, arrivals):
    copies = [
        pltpu.make_async_copy(volts_out, volts, arrivals.at[2]),
        pltpu.make_async_copy(fixed, fixed_here, arrivals.at[0]),
        pltpu.make_async_copy(gate, gate_here, arrivals.at[1]),
    ]
    later = []
    for n in range(3):
        start = pl.multiple_of(jnp.clip(energy[0] + n - 1, 0, NE - 1) * LD, LD)
        later.append(
            pltpu.make_async_copy(cells.at[pl.ds(start, LD)], near.at[pl.ds(n * LD, LD)], arrivals.at[3 + n])
        )
    for copy in copies + later:
        copy.start()
    for copy in copies:
        copy.wait()
    for out, planes in ((xup, (PLANES - 2, PLANES - 1)), (xdown, (0, 1))):
        for i, p in enumerate(planes):
            g = gate_here[p].astype(jnp.float32)
            out[i] = fixed_here[p] + PENALTY * g * volts[p]
            if p in (0, PLANES - 1):
                out[2] = g

    def one_plane(p, carry):
        volt = PENALTY * volts[p]
        for out, rows in ((yup, (CY - 2, CY - 1)), (ydown, (0, 1))):
            for i, y in enumerate(rows):
                g = gate_here[p, y : y + 1, :].astype(jnp.float32)
                out[i, pl.ds(p, 1), :] = fixed_here[p, y : y + 1, :] + volt * g
                if y in (0, CY - 1):
                    out[2, pl.ds(p, 1), :] = g
        return carry

    lax.fori_loop(0, PLANES, one_plane, 0, unroll=8)
    for copy in later:
        copy.wait()


def edges(e, volts, fixed, gate, cells):
    shapes = [(3, CY, NZ)] * 2 + [(3, PLANES, NZ)] * 2
    hbm = pl.BlockSpec(memory_space=pltpu.HBM)
    return pl.pallas_call(
        edges_body,
        grid_spec=pltpu.PrefetchScalarGridSpec(
            num_scalar_prefetch=1,
            grid=(1,),
            in_specs=[hbm, hbm, hbm, hbm],
            out_specs=[pl.BlockSpec(x, lambda i, *_: (0, 0, 0)) for x in shapes]
            + [pl.BlockSpec((3 * LD, ORB), lambda i, *_: (0, 0))],
            scratch_shapes=[
                pltpu.VMEM((PLANES, CY, NZ), jnp.float32),
                pltpu.VMEM((PLANES, CY, NZ), jnp.int32),
                pltpu.SMEM((PLANES,), jnp.float32),
                pltpu.SemaphoreType.DMA((6,)),
            ],
        ),
        out_shape=[jax.ShapeDtypeStruct(x, jnp.float32) for x in shapes]
        + [jax.ShapeDtypeStruct((3 * LD, ORB), jnp.int32)],
        compiler_params=params(8),
        name="edges",
    )(e[None], in_hbm(volts), in_hbm(fixed), in_hbm(gate), in_hbm(cells))


def collect_body(energy, kpt, parts, out, corners):
    e = energy[0]
    k = kpt[0]
    total = parts[0]
    for i in range(1, NE * NZC):
        total = total + parts[i]
    for n in range(NK):
        out[n] = total
    for i, dx in enumerate((-1, 1)):
        for j, dy in enumerate((-1, 1)):
            from_e = e + dx
            from_k = k + dy
            there = (from_e >= 0) & (from_e < NE) & (from_k >= 0) & (from_k < NK)
            source = jnp.where(there, from_e * NZC + from_k // 2, 0)
            lines = parts[source, 30:32, :]
            corners[i, j : j + 1, 0:128] = jnp.where(there, lines[0:1], 0.0)
            corners[i, j : j + 1, 128:256] = jnp.where(there, lines[1:2], 0.0)


def collect(e, k, parts):
    whole = lambda shape: pl.BlockSpec(shape, lambda i, *_: (0, 0, 0))
    shapes = [(NK, 32, 128), (2, 2, NZ)]
    return pl.pallas_call(
        collect_body,
        grid_spec=pltpu.PrefetchScalarGridSpec(
            num_scalar_prefetch=2,
            grid=(1,),
            in_specs=[whole((NE * NZC, 32, 128))],
            out_specs=[whole(x) for x in shapes],
        ),
        out_shape=[jax.ShapeDtypeStruct(x, jnp.float32) for x in shapes],
        compiler_params=params(4),
        name="collect",
    )(e[None], k[None], parts)


def split_parts(x):
    high = x.astype(jnp.bfloat16)
    low = (x - high.astype(jnp.float32)).astype(jnp.bfloat16)
    return high, low


def spread(line, rows):
    block = jnp.broadcast_to(line, (16, 128)).astype(jnp.bfloat16)
    return jnp.concatenate([block] * (rows // 16), axis=0)


def counting(rows):
    return lax.broadcasted_iota(jnp.int32, (rows, 128), 0).astype(jnp.float32).astype(jnp.bfloat16)


def tiles_of(line):
    return [line[:, 128 * t : 128 * (t + 1)] for t in range(line.shape[1] // 128)]


def marks(index, rows, counts):
    one = jnp.ones((), jnp.bfloat16)
    zero = jnp.zeros((), jnp.bfloat16)
    return jnp.concatenate([jnp.where(counts[:rows] == spread(t, rows), one, zero) for t in tiles_of(index)], axis=1)


def charge_of(cells, values, first_plane, planes, y0):
    plane = (cells >> 15) - first_plane
    dy = ((cells >> 8) & (NY - 1)) - y0
    near = (dy >= -2) & (dy < CY + 2) & (plane >= 0) & (plane < planes)
    row = jnp.where(near, plane * WC + jnp.where(dy >= 0, dy, dy + WC), -1).astype(jnp.float32)
    z = (cells & (NZ - 1)).astype(jnp.float32)
    rows = planes * WC
    padded = -(-rows // 16) * 16
    counts = counting(NZ)
    high = values.astype(jnp.bfloat16).astype(jnp.float32)
    low = values - high
    zero = jnp.zeros((), jnp.bfloat16)
    tops, bottoms = [], []
    for t, h, l in zip(tiles_of(row), tiles_of(high), tiles_of(low)):
        hit = counts[:padded] == spread(t, padded)
        tops.append(jnp.where(hit, spread(h, padded), zero))
        bottoms.append(jnp.where(hit, spread(l, padded), zero))
    left = jnp.concatenate([jnp.concatenate(tops, axis=1), jnp.concatenate(bottoms, axis=1)], axis=0)
    right = marks(z, NZ, counts)
    both = lax.dot_general(left, right, (((1,), (1,)), ((), ())), preferred_element_type=jnp.float32)
    return both[:padded] + both[padded:]


def in_plane(here):
    lane = lax.broadcasted_iota(jnp.int32, (W, NZ), 1)
    total = pltpu.roll(here, 1, 0) + pltpu.roll(here, W - 1, 0)
    total = total + jnp.where(lane == 0, 0.0, pltpu.roll(here, 1, 1))
    return total + jnp.where(lane == NZ - 1, 0.0, pltpu.roll(here, NZ - 1, 1))


def field_body(energy, kpt, occ, cells, corners, xlow, xhigh, ylow, yhigh, volts_out, fixed, gate,
               sums, fields_out, r_ext, g_ext, fixed_here, gate_here, volts, arrivals):
    e = energy[0]
    k = kpt[0]
    y0 = k * CY
    copies = [
        pltpu.make_async_copy(volts_out, volts, arrivals.at[2]),
        pltpu.make_async_copy(fixed, fixed_here, arrivals.at[0]),
        pltpu.make_async_copy(gate, gate_here, arrivals.at[1]),
    ]
    for copy in copies:
        copy.start()
    row = lax.broadcasted_iota(jnp.int32, (W, NZ), 0)
    y = jnp.where(row < CY + 4, row, row - W) + y0
    valid = jnp.where((y >= 0) & (y < NY), 1.0, 0.0)

    def values_of(index):
        return jnp.concatenate(
            [occ[c, pl.ds(index(t), 1), :] for c in range(NK) for t in range(TL)], axis=1
        )

    gap = jnp.zeros((4, NZ), jnp.float32)

    def keep(charge, planes, at):
        for p in range(planes):
            r_ext[at + p, 0:CY, :] = -charge[WC * p : WC * p + CY]
            r_ext[at + p, CY : CY + 2, :] = -charge[WC * p + CY : WC * p + CY + 2]
            r_ext[at + p, CY + 2 : W - 2, :] = gap
            r_ext[at + p, W - 2 : W, :] = -charge[WC * p + CY + 2 : WC * p + WC]

    for j in range(LD):
        charge = charge_of(cells[LD + j : LD + j + 1, :], values_of(lambda t: 8 * t + j), 0, SUB, y0)
        keep(charge, SUB, 2 + SUB * j)
    keep(charge_of(cells[LD - 1 : LD, :], values_of(lambda t: 24 + t), SUB - 2, 2, y0), 2, 0)
    keep(charge_of(cells[2 * LD : 2 * LD + 1, :], values_of(lambda t: 27 + t), 0, 2, y0), 2, PLANES + 2)

    for at, halo in ((0, xlow), (PLANES + 2, xhigh)):
        for i in range(2):
            r_ext[at + i, 0:CY, :] = r_ext[at + i, 0:CY, :] + halo[i]
    g_ext[1, 0:CY, :] = xlow[2]
    g_ext[PLANES + 2, 0:CY, :] = xhigh[2]
    sub = lax.broadcasted_iota(jnp.int32, (8, NZ), 0)
    none = jnp.zeros((8, NZ), jnp.float32)
    line = lambda x: jnp.broadcast_to(x, (8, NZ))
    for at, i in ((1, 0), (PLANES + 2, 1)):
        tile = jnp.where(sub == 0, line(corners[i, 1:2, :]), jnp.where(sub == 7, line(corners[i, 0:1, :]), none))
        r_ext[at, CY:W, :] = r_ext[at, CY:W, :] + tile
        g_ext[at, CY:W, :] = none
    for copy in copies:
        copy.wait()

    def load_plane(p, carry):
        at = pl.ds(p, 1)
        g = gate_here[p].astype(jnp.float32)
        g_ext[p + 2, 0:CY, :] = g
        r_ext[p + 2, 0:CY, :] = r_ext[p + 2, 0:CY, :] + (fixed_here[p] + PENALTY * g * volts[p])
        tile = jnp.where(sub == 0, line(yhigh[0, at, :]), jnp.where(sub == 1, line(yhigh[1, at, :]), none))
        tile = jnp.where(sub == 6, line(ylow[0, at, :]), jnp.where(sub == 7, line(ylow[1, at, :]), tile))
        r_ext[p + 2, CY:W, :] = r_ext[p + 2, CY:W, :] + tile
        tile = jnp.where(sub == 0, line(yhigh[2, at, :]), jnp.where(sub == 7, line(ylow[2, at, :]), none))
        g_ext[p + 2, CY:W, :] = tile
        return carry

    lax.fori_loop(0, PLANES, load_plane, 0, unroll=8)

    def image_plane(p):
        here = r_ext[p + 1]
        x = e * PLANES + p - 1
        inside = jnp.where((x >= 0) & (x < NE * PLANES), 1.0, 0.0)
        around = r_ext[p + 2] + r_ext[p] + in_plane(here)
        return ((6.0 + PENALTY * g_ext[p + 1]) * here - around) * (valid * inside)

    def sum_plane(p, carry):
        before, here, rr, rw, ww, waw = carry
        after = image_plane(p + 2)
        r = r_ext[p + 2, 0:CY, :]
        w = here[0:CY]
        image = ((6.0 + PENALTY * g_ext[p + 2]) * here - (before + after + in_plane(here)))[0:CY]
        fields_out[0, p] = r
        fields_out[1, p] = w
        return here, after, rr + r * r, rw + r * w, ww + w * w, waw + w * image

    zero = jnp.zeros((CY, NZ), jnp.float32)
    totals = lax.fori_loop(0, PLANES, sum_plane, (image_plane(0), image_plane(1)) + (zero,) * 4, unroll=8)[2:]
    lane = lax.broadcasted_iota(jnp.int32, (1, 128), 1)
    line = jnp.zeros((1, 128), jnp.float32)
    for i, total in enumerate(totals):
        line = line + jnp.where(lane == i, jnp.sum(total), 0.0)
    for d in range(NE * NK):
        sums[d] = line


def fields(e, k, volts, occ, cells, corners, fixed, gate, xlow, xhigh, ylow, yhigh):
    whole = lambda x: pl.BlockSpec(x.shape, lambda i, *_: (0,) * x.ndim)
    shapes = [
        jax.ShapeDtypeStruct((NE * NK, 1, 128), jnp.float32),
        jax.ShapeDtypeStruct((2, PLANES, CY, NZ), jnp.float32),
    ]
    return pl.pallas_call(
        field_body,
        grid_spec=pltpu.PrefetchScalarGridSpec(
            num_scalar_prefetch=2,
            grid=(1,),
            in_specs=[whole(x) for x in (occ, cells, corners, xlow, xhigh, ylow, yhigh)]
            + [pl.BlockSpec(memory_space=pltpu.HBM)] * 3,
            out_specs=[
                pl.BlockSpec((NE * NK, 1, 128), lambda i, *_: (0, 0, 0)),
                pl.BlockSpec((2, PLANES, CY, NZ), lambda i, *_: (0, 0, 0, 0)),
            ],
            scratch_shapes=[
                pltpu.VMEM((PLANES + 4, W, NZ), jnp.float32),
                pltpu.VMEM((PLANES + 4, W, NZ), jnp.float32),
                pltpu.VMEM((PLANES, CY, NZ), jnp.float32),
                pltpu.VMEM((PLANES, CY, NZ), jnp.int32),
                pltpu.SMEM((PLANES,), jnp.float32),
                pltpu.SemaphoreType.DMA((3,)),
            ],
        ),
        out_shape=shapes,
        compiler_params=params(16),
        name="fields",
    )(e[None], k[None], occ, cells, corners, xlow, xhigh, ylow, yhigh, in_hbm(volts), in_hbm(fixed), in_hbm(gate))


def lengths(sums):
    line = jnp.sum(sums[...].reshape(NE * NK, 128), axis=0, keepdims=True)
    lane = lax.broadcasted_iota(jnp.int32, (1, 128), 1)
    rr, rw, ww, waw = [
        jnp.broadcast_to(jnp.sum(jnp.where(lane == i, line, 0.0), axis=1, keepdims=True), (1, NZ)) for i in range(4)
    ]
    alpha = rr / rw
    norm = alpha * alpha * ww - rr
    ratio = norm / rr
    ahead = 1.0 + ratio
    curve = ahead * ahead * rw - 2.0 * ahead * alpha * ww + alpha * alpha * waw
    small = (norm <= 1e-9 * rr) | (curve <= 0.0)
    step = jnp.where(small, alpha, norm / curve)
    ahead = jnp.where(small, 1.0, ahead)
    return alpha + step * ahead, -alpha * step


def pick_body(kpt, sums, cells_near, rw, out, grid_out, grid_here, leaving):
    y0 = kpt[0] * CY
    wide = 2 * COL
    counts = counting(NZ)
    c_r, c_w = [jnp.broadcast_to(c, (SUB * CY, NZ)) for c in lengths(sums)]
    copies = []
    for j in range(LD):
        at = pl.ds(SUB * j, SUB)
        field = c_r * rw[0, at].reshape(SUB * CY, NZ) + c_w * rw[1, at].reshape(SUB * CY, NZ)
        grid_here[at] = field.reshape(SUB, CY, NZ)
        copies.append(pltpu.make_async_copy(grid_here.at[at], grid_out.at[at], leaving.at[j]))
        copies[-1].start()
        high, low = split_parts(field)
        for n in range(ORB // wide):
            cells = cells_near[LD + j : LD + j + 1, n * wide : (n + 1) * wide]
            dy = ((cells >> 8) & (NY - 1)) - y0
            row = jnp.where((dy >= 0) & (dy < CY), (cells >> 15) * CY + dy, -1)
            z = cells & (NZ - 1)
            right = marks(z.astype(jnp.float32), NZ, counts)
            lines = jnp.dot(high, right, preferred_element_type=jnp.float32)
            lines = lines + jnp.dot(low, right, preferred_element_type=jnp.float32)
            hit = lax.broadcasted_iota(jnp.int32, (SUB * CY, wide), 0) == row
            value = jnp.sum(jnp.where(hit, lines, 0.0), axis=0, keepdims=True)
            for h in range(2):
                out[2 * n + h, j : j + 1, :] = value[:, h * COL : (h + 1) * COL]
    for copy in copies:
        copy.wait()


def pick(k, sums, cells, rw):
    whole = lambda shape: pl.BlockSpec(shape, lambda i, *_: (0,) * len(shape))
    shape = jax.ShapeDtypeStruct((NK, LD, COL), jnp.float32)
    return pl.pallas_call(
        pick_body,
        grid_spec=pltpu.PrefetchScalarGridSpec(
            num_scalar_prefetch=1,
            grid=(1,),
            in_specs=[whole(sums.shape), whole(cells.shape), whole(rw.shape)],
            out_specs=[whole(shape.shape), pl.BlockSpec(memory_space=pltpu.HBM)],
            scratch_shapes=[pltpu.VMEM((PLANES, CY, NZ), jnp.float32), pltpu.SemaphoreType.DMA((LD,))],
        ),
        out_shape=[shape, pltpu.HBM((PLANES, CY, NZ), jnp.float32)],
        compiler_params=params(12),
        name="pick",
    )(k[None], sums, cells, rw)


def join_body(picked, out):
    total = picked[0]
    for i in range(1, NK):
        total = total + picked[i]
    for d in range(NE * NZC):
        out[d] = total


def join(picked):
    return pl.pallas_call(
        join_body,
        out_shape=jax.ShapeDtypeStruct((NE * NZC, LD, COL), jnp.float32),
        compiler_params=params(4),
        name="join",
    )(picked)


def band_body(which, density, values, before, out, acc):
    z = pl.program_id(0)
    start = pl.multiple_of(which[0] * COL, 128)

    @pl.when(z == 0)
    def _():
        acc[...] = jnp.zeros_like(acc)

    for m in range(0, NE, 2):
        v = values[m : m + 2, 0].reshape(16, COL)
        for i in range(EL):
            part = density[i, 8 * m : 8 * m + 16, pl.ds(start, COL)].astype(jnp.float32) * v
            total = part[:, :128]
            for t in range(1, TL):
                total = total + part[:, 128 * t : 128 * (t + 1)]
            acc[i, 8 * m : 8 * m + 16] = acc[i, 8 * m : 8 * m + 16] + total

    @pl.when(z == NZC - 1)
    def _():
        for i in range(EL):
            out[i : i + 1, :] = before[i : i + 1, :] + jnp.sum(acc[i].T, axis=0, keepdims=True) * ORB**-0.5


def band(which, density, values, before):
    small = pl.BlockSpec((EL, LAYERS), lambda z, *_: (0, 0))
    return pl.pallas_call(
        band_body,
        grid_spec=pltpu.PrefetchScalarGridSpec(
            num_scalar_prefetch=1,
            grid=(NZC,),
            in_specs=[
                pl.BlockSpec((EL, LAYERS, 2 * COL), lambda z, *_: (0, 0, z)),
                pl.BlockSpec((NE, 1, LD, COL), lambda z, *_: (0, z, 0, 0)),
                small,
            ],
            out_specs=small,
            scratch_shapes=[pltpu.VMEM((EL, LAYERS, 128), jnp.float32)],
        ),
        out_shape=jax.ShapeDtypeStruct((EL, LAYERS), jnp.float32),
        compiler_params=params(8),
        name="band",
    )(which, density, values, before)


def shift_up(x, axis):
    return lax.ppermute(x, axis, [(i, i + 1) for i in range(lax.axis_size(axis) - 1)])


def shift_down(x, axis):
    return lax.ppermute(x, axis, [(i + 1, i) for i in range(lax.axis_size(axis) - 1)])


def one_step(density, quad_weights, orbital_cells, fixed_charge, gate_mask, gate_voltage):
    e = lax.axis_index(ENERGY).astype(jnp.int32)
    k = lax.axis_index(KPT).astype(jnp.int32)
    core = lax.axis_index(CORE).astype(jnp.int32)[None]
    density = density.reshape(EL, LAYERS, ORB)

    own, other = occupancy_parts(e, k, gate_voltage, quad_weights.reshape(1, EL), density, fixed_charge, gate_mask)
    chips = NE * NZC
    received = swap_cores(other.reshape(chips, 32, 128))
    xup, xdown, yup, ydown, cells = edges(e, gate_voltage, fixed_charge, gate_mask, orbital_cells)
    pair = own.reshape(chips, 32, 128) + received
    parts = exchange(pair, CHIPS)
    xlow = shift_up(xup, ENERGY)
    xhigh = shift_down(xdown, ENERGY)
    ylow = shift_up(yup, KPT)
    yhigh = shift_down(ydown, KPT)
    parts, xlow, xhigh = lax.optimization_barrier((parts, xlow, xhigh))
    occ, corners = collect(e, k, parts)
    occ = exchange(occ, KPT)
    sums, rw = fields(
        e, k, gate_voltage, occ, cells, corners, fixed_charge, gate_mask, xlow, xhigh, ylow, yhigh
    )
    all_sums = exchange(sums, EVERY)
    picked, potential = pick(k, all_sums, cells, rw)
    picked = exchange(picked, KPT)
    same = exchange(join(picked), CHIPS)
    shape = (NE, NZC, LD, COL)
    cross = swap_cores(same)
    shift = band(core, density, same.reshape(shape), jnp.zeros((EL, LAYERS), jnp.float32))
    shift = band(1 - core, density, cross.reshape(shape), shift)
    return potential, shift.reshape(EL, 1, LAYERS)


def solution(mesh):
    split = Mesh(mesh.devices.reshape(4, 4, 4, 2), ("energy_0", "energy_1", "kpt_0", "kpt_1"))
    in_specs = (
        P(ENERGY, KPT, None, None),
        P(ENERGY, KPT),
        P(),
        P(ENERGY, KPT, None),
        P(ENERGY, KPT, None),
        P(ENERGY),
    )
    out_specs = (P(ENERGY, KPT, None), P(ENERGY, KPT, None))
    return jax.shard_map(one_step, mesh=split, in_specs=in_specs, out_specs=out_specs, check_vma=False)
```

```python
import jax
import jax.numpy as jnp
from jax import lax
from jax.experimental import pallas as pl
from jax.experimental.pallas import tpu as pltpu
from jax.sharding import Mesh
from jax.sharding import PartitionSpec as P

ENERGY = ("energy_0", "energy_1")
KPT = ("kpt_0", "kpt_1")
CHIPS = ("energy_0", "energy_1", "kpt_0")
CORE = "kpt_1"
EVERY = ("energy_0", "energy_1", "kpt_0", "kpt_1")

NE = 16
NK = 8
NZC = 4
SUB = 8
LAYERS = 128
LD = 8
ORB = 3072
CY = 16
NY = 128
NZ = 256
PLANES = 64
EL = 4
W = 24
WC = 20
COL = ORB // NK
TL = COL // 128
PENALTY = 4.0
AHEAD = 4


def swap_cores(x):
    return lax.ppermute(x, CORE, [(0, 1), (1, 0)])


def exchange(x, axis):
    return lax.all_to_all(x, axis, split_axis=0, concat_axis=0, tiled=True)


def in_hbm(x):
    return pltpu.with_memory_space_constraint(x, pltpu.HBM)


def params(mib):
    return pltpu.CompilerParams(vmem_limit_bytes=mib * 1024 * 1024)


def occupancy_body(energy, kpt, weights_out, density_out, volts_out, fixed, gate, own, other,
                   weights, density, fixed_ends, gate_ends, volts, arrivals, blocks):
    e = energy[0]
    k = kpt[0]
    core = k % 2
    small = [
        pltpu.make_async_copy(weights_out, weights, arrivals.at[0]),
        pltpu.make_async_copy(volts_out, volts, arrivals.at[1]),
    ]
    for i, plane in enumerate((0, PLANES - 1)):
        small.append(pltpu.make_async_copy(fixed.at[plane], fixed_ends.at[i], arrivals.at[2 + 2 * i]))
        small.append(pltpu.make_async_copy(gate.at[plane], gate_ends.at[i], arrivals.at[3 + 2 * i]))
    large = [
        pltpu.make_async_copy(density_out.at[:, :, pl.ds(2 * COL * z, 2 * COL)], density.at[z], blocks.at[z])
        for z in range(NZC)
    ]
    for copy in small[:1] + large[:AHEAD] + small[1:]:
        copy.start()
    small[0].wait()
    scale = [jnp.broadcast_to(weights[0:1, n : n + 1], (16, COL)) for n in range(EL)]
    zero = jnp.zeros((3, 128), jnp.float32)
    for z in range(NZC):
        large[z].wait()
        if z + AHEAD < NZC:
            large[z + AHEAD].start()
        for half, out in ((0, own), (1, other)):
            which = core if half == 0 else 1 - core
            start = pl.multiple_of(which * COL, 128)
            for i in range(0, NE, 2):
                total = None
                for n in range(EL):
                    part = density[z, n, 8 * i : 8 * i + 16, pl.ds(start, COL)].astype(jnp.float32) * scale[n]
                    total = part if total is None else total + part
                for h in range(2):
                    at = i + h
                    for t in range(TL):
                        tile = total[8 * h : 8 * h + 8, 128 * t : 128 * (t + 1)]
                        out[at, z, 8 * t : 8 * t + 8, :] = tile
                        if at + 1 < NE:
                            out[at + 1, z, 24 + t : 25 + t, :] = tile[7:8]
                        if at > 0:
                            out[at - 1, z, 27 + t : 28 + t, :] = tile[0:1]
            out[0, z, 24:27, :] = zero
            out[NE - 1, z, 27:30, :] = zero
            for i in range(NE):
                out[i, z, 30:32, :] = zero[:2]
    for copy in small[1:]:
        copy.wait()

    for dx in (-1, 1):
        for dy in (-1, 1):
            to_e = e + dx
            to_k = k + dy

            @pl.when((to_e >= 0) & (to_e < NE) & (to_k >= 0) & (to_k < NK))
            def _(dx=dx, dy=dy, to_e=to_e, to_k=to_k):
                i = 1 if dx == 1 else 0
                y = CY - 1 if dy == 1 else 0
                g = gate_ends[i, y : y + 1, :].astype(jnp.float32)
                line = fixed_ends[i, y : y + 1, :] + PENALTY * g * volts[(PLANES - 1) * i]
                other[to_e, to_k // 2, 30:31, :] = line[:, :128]
                other[to_e, to_k // 2, 31:32, :] = line[:, 128:]


def occupancy_parts(e, k, volts, weights, density, fixed, gate):
    shape = (NE, NZC, 32, 128)
    hbm = pl.BlockSpec(memory_space=pltpu.HBM)
    return pl.pallas_call(
        occupancy_body,
        grid_spec=pltpu.PrefetchScalarGridSpec(
            num_scalar_prefetch=2,
            grid=(1,),
            in_specs=[hbm] * 5,
            out_specs=[pl.BlockSpec(shape, lambda i, *_: (0, 0, 0, 0))] * 2,
            scratch_shapes=[
                pltpu.VMEM((1, EL), jnp.float32),
                pltpu.VMEM((NZC, EL, LAYERS, 2 * COL), jnp.bfloat16),
                pltpu.VMEM((2, CY, NZ), jnp.float32),
                pltpu.VMEM((2, CY, NZ), jnp.int32),
                pltpu.SMEM((PLANES,), jnp.float32),
                pltpu.SemaphoreType.DMA((6,)),
                pltpu.SemaphoreType.DMA((NZC,)),
            ],
        ),
        out_shape=[jax.ShapeDtypeStruct(shape, jnp.float32)] * 2,
        compiler_params=params(10),
        name="occupancy_parts",
    )(e[None], k[None], in_hbm(weights), in_hbm(density), in_hbm(volts), in_hbm(fixed), in_hbm(gate))


def edges_body(energy, volts_out, fixed, gate, cells, xup, xdown, yup, ydown, near, fixed_here, gate_here, volts, arrivals):
    copies = [
        pltpu.make_async_copy(volts_out, volts, arrivals.at[2]),
        pltpu.make_async_copy(fixed, fixed_here, arrivals.at[0]),
        pltpu.make_async_copy(gate, gate_here, arrivals.at[1]),
    ]
    later = []
    for n in range(3):
        start = pl.multiple_of(jnp.clip(energy[0] + n - 1, 0, NE - 1) * LD, LD)
        later.append(
            pltpu.make_async_copy(cells.at[pl.ds(start, LD)], near.at[pl.ds(n * LD, LD)], arrivals.at[3 + n])
        )
    for copy in copies + later:
        copy.start()
    for copy in copies:
        copy.wait()
    for out, planes in ((xup, (PLANES - 2, PLANES - 1)), (xdown, (0, 1))):
        for i, p in enumerate(planes):
            g = gate_here[p].astype(jnp.float32)
            out[i] = fixed_here[p] + PENALTY * g * volts[p]
            if p in (0, PLANES - 1):
                out[2] = g

    def one_plane(p, carry):
        volt = PENALTY * volts[p]
        for out, rows in ((yup, (CY - 2, CY - 1)), (ydown, (0, 1))):
            for i, y in enumerate(rows):
                g = gate_here[p, y : y + 1, :].astype(jnp.float32)
                out[i, pl.ds(p, 1), :] = fixed_here[p, y : y + 1, :] + volt * g
                if y in (0, CY - 1):
                    out[2, pl.ds(p, 1), :] = g
        return carry

    lax.fori_loop(0, PLANES, one_plane, 0, unroll=8)
    for copy in later:
        copy.wait()


def edges(e, volts, fixed, gate, cells):
    shapes = [(3, CY, NZ)] * 2 + [(3, PLANES, NZ)] * 2
    hbm = pl.BlockSpec(memory_space=pltpu.HBM)
    return pl.pallas_call(
        edges_body,
        grid_spec=pltpu.PrefetchScalarGridSpec(
            num_scalar_prefetch=1,
            grid=(1,),
            in_specs=[hbm, hbm, hbm, hbm],
            out_specs=[pl.BlockSpec(x, lambda i, *_: (0, 0, 0)) for x in shapes]
            + [pl.BlockSpec((3 * LD, ORB), lambda i, *_: (0, 0))],
            scratch_shapes=[
                pltpu.VMEM((PLANES, CY, NZ), jnp.float32),
                pltpu.VMEM((PLANES, CY, NZ), jnp.int32),
                pltpu.SMEM((PLANES,), jnp.float32),
                pltpu.SemaphoreType.DMA((6,)),
            ],
        ),
        out_shape=[jax.ShapeDtypeStruct(x, jnp.float32) for x in shapes]
        + [jax.ShapeDtypeStruct((3 * LD, ORB), jnp.int32)],
        compiler_params=params(8),
        name="edges",
    )(e[None], in_hbm(volts), in_hbm(fixed), in_hbm(gate), in_hbm(cells))


def collect_body(energy, kpt, parts, out, corners):
    e = energy[0]
    k = kpt[0]
    total = parts[0]
    for i in range(1, NE * NZC):
        total = total + parts[i]
    for n in range(NK):
        out[n] = total
    for i, dx in enumerate((-1, 1)):
        for j, dy in enumerate((-1, 1)):
            from_e = e + dx
            from_k = k + dy
            there = (from_e >= 0) & (from_e < NE) & (from_k >= 0) & (from_k < NK)
            source = jnp.where(there, from_e * NZC + from_k // 2, 0)
            lines = parts[source, 30:32, :]
            corners[i, j : j + 1, 0:128] = jnp.where(there, lines[0:1], 0.0)
            corners[i, j : j + 1, 128:256] = jnp.where(there, lines[1:2], 0.0)


def collect(e, k, parts):
    whole = lambda shape: pl.BlockSpec(shape, lambda i, *_: (0, 0, 0))
    shapes = [(NK, 32, 128), (2, 2, NZ)]
    return pl.pallas_call(
        collect_body,
        grid_spec=pltpu.PrefetchScalarGridSpec(
            num_scalar_prefetch=2,
            grid=(1,),
            in_specs=[whole((NE * NZC, 32, 128))],
            out_specs=[whole(x) for x in shapes],
        ),
        out_shape=[jax.ShapeDtypeStruct(x, jnp.float32) for x in shapes],
        compiler_params=params(4),
        name="collect",
    )(e[None], k[None], parts)


def split_parts(x):
    high = x.astype(jnp.bfloat16)
    low = (x - high.astype(jnp.float32)).astype(jnp.bfloat16)
    return high, low


def spread(line, rows):
    block = jnp.broadcast_to(line, (16, 128)).astype(jnp.bfloat16)
    return jnp.concatenate([block] * (rows // 16), axis=0)


def counting(rows):
    return lax.broadcasted_iota(jnp.int32, (rows, 128), 0).astype(jnp.float32).astype(jnp.bfloat16)


def tiles_of(line):
    return [line[:, 128 * t : 128 * (t + 1)] for t in range(line.shape[1] // 128)]


def marks(index, rows, counts):
    one = jnp.ones((), jnp.bfloat16)
    zero = jnp.zeros((), jnp.bfloat16)
    return jnp.concatenate([jnp.where(counts[:rows] == spread(t, rows), one, zero) for t in tiles_of(index)], axis=1)


def charge_of(cells, values, first_plane, planes, y0):
    plane = (cells >> 15) - first_plane
    dy = ((cells >> 8) & (NY - 1)) - y0
    near = (dy >= -2) & (dy < CY + 2) & (plane >= 0) & (plane < planes)
    row = jnp.where(near, plane * WC + jnp.where(dy >= 0, dy, dy + WC), -1).astype(jnp.float32)
    z = (cells & (NZ - 1)).astype(jnp.float32)
    rows = planes * WC
    padded = -(-rows // 16) * 16
    counts = counting(NZ)
    high = values.astype(jnp.bfloat16).astype(jnp.float32)
    low = values - high
    zero = jnp.zeros((), jnp.bfloat16)
    tops, bottoms = [], []
    for t, h, l in zip(tiles_of(row), tiles_of(high), tiles_of(low)):
        hit = counts[:padded] == spread(t, padded)
        tops.append(jnp.where(hit, spread(h, padded), zero))
        bottoms.append(jnp.where(hit, spread(l, padded), zero))
    left = jnp.concatenate([jnp.concatenate(tops, axis=1), jnp.concatenate(bottoms, axis=1)], axis=0)
    right = marks(z, NZ, counts)
    both = lax.dot_general(left, right, (((1,), (1,)), ((), ())), preferred_element_type=jnp.float32)
    return both[:padded] + both[padded:]


def in_plane(here):
    lane = lax.broadcasted_iota(jnp.int32, (W, NZ), 1)
    total = pltpu.roll(here, 1, 0) + pltpu.roll(here, W - 1, 0)
    total = total + jnp.where(lane == 0, 0.0, pltpu.roll(here, 1, 1))
    return total + jnp.where(lane == NZ - 1, 0.0, pltpu.roll(here, NZ - 1, 1))


def field_body(energy, kpt, occ, cells, corners, xlow, xhigh, ylow, yhigh, volts_out, fixed, gate,
               sums, fields_out, r_ext, g_ext, fixed_here, gate_here, volts, arrivals):
    e = energy[0]
    k = kpt[0]
    y0 = k * CY
    copies = [
        pltpu.make_async_copy(volts_out, volts, arrivals.at[2]),
        pltpu.make_async_copy(fixed, fixed_here, arrivals.at[0]),
        pltpu.make_async_copy(gate, gate_here, arrivals.at[1]),
    ]
    for copy in copies:
        copy.start()
    row = lax.broadcasted_iota(jnp.int32, (W, NZ), 0)
    y = jnp.where(row < CY + 4, row, row - W) + y0
    valid = jnp.where((y >= 0) & (y < NY), 1.0, 0.0)

    def values_of(index):
        return jnp.concatenate(
            [occ[c, pl.ds(index(t), 1), :] for c in range(NK) for t in range(TL)], axis=1
        )

    gap = jnp.zeros((4, NZ), jnp.float32)

    def keep(charge, planes, at):
        for p in range(planes):
            r_ext[at + p, 0:CY, :] = -charge[WC * p : WC * p + CY]
            r_ext[at + p, CY : CY + 2, :] = -charge[WC * p + CY : WC * p + CY + 2]
            r_ext[at + p, CY + 2 : W - 2, :] = gap
            r_ext[at + p, W - 2 : W, :] = -charge[WC * p + CY + 2 : WC * p + WC]

    keep(charge_of(cells[LD - 1 : LD, :], values_of(lambda t: 24 + t), SUB - 2, 2, y0), 2, 0)
    keep(charge_of(cells[2 * LD : 2 * LD + 1, :], values_of(lambda t: 27 + t), 0, 2, y0), 2, PLANES + 2)
    for at, halo in ((0, xlow), (PLANES + 2, xhigh)):
        for i in range(2):
            r_ext[at + i, 0:CY, :] = r_ext[at + i, 0:CY, :] + halo[i]
    g_ext[1, 0:CY, :] = xlow[2]
    g_ext[PLANES + 2, 0:CY, :] = xhigh[2]
    sub = lax.broadcasted_iota(jnp.int32, (8, NZ), 0)
    none = jnp.zeros((8, NZ), jnp.float32)
    wide = lambda x: jnp.broadcast_to(x, (8, NZ))
    for at, i in ((1, 0), (PLANES + 2, 1)):
        tile = jnp.where(sub == 0, wide(corners[i, 1:2, :]), jnp.where(sub == 7, wide(corners[i, 0:1, :]), none))
        r_ext[at, CY:W, :] = r_ext[at, CY:W, :] + tile
        g_ext[at, CY:W, :] = none
    for copy in copies:
        copy.wait()

    def load_plane(p):
        at = slice(p, p + 1)
        g = gate_here[p].astype(jnp.float32)
        g_ext[p + 2, 0:CY, :] = g
        r_ext[p + 2, 0:CY, :] = r_ext[p + 2, 0:CY, :] + (fixed_here[p] + PENALTY * g * volts[p])
        tile = jnp.where(sub == 0, wide(yhigh[0, at, :]), jnp.where(sub == 1, wide(yhigh[1, at, :]), none))
        tile = jnp.where(sub == 6, wide(ylow[0, at, :]), jnp.where(sub == 7, wide(ylow[1, at, :]), tile))
        r_ext[p + 2, CY:W, :] = r_ext[p + 2, CY:W, :] + tile
        tile = jnp.where(sub == 0, wide(yhigh[2, at, :]), jnp.where(sub == 7, wide(ylow[2, at, :]), none))
        g_ext[p + 2, CY:W, :] = tile

    def image_plane(p):
        here = r_ext[p + 1]
        inside = valid
        if p in (0, PLANES + 1):
            x = e * PLANES + p - 1
            inside = valid * jnp.where((x >= 0) & (x < NE * PLANES), 1.0, 0.0)
        around = r_ext[p + 2] + r_ext[p] + in_plane(here)
        return ((6.0 + PENALTY * g_ext[p + 1]) * here - around) * inside

    def sum_plane(p, carry):
        before, here, rr, rw, ww, waw = carry
        after = image_plane(p + 2)
        r = r_ext[p + 2, 0:CY, :]
        w = here[0:CY]
        image = ((6.0 + PENALTY * g_ext[p + 2]) * here - (before + after + in_plane(here)))[0:CY]
        fields_out[0, p] = r
        fields_out[1, p] = w
        return here, after, rr + r * r, rw + r * w, ww + w * w, waw + w * image

    carry = None
    done = 0
    for j in range(LD + 1):
        if j < LD:
            charge = charge_of(cells[LD + j : LD + j + 1, :], values_of(lambda t: 8 * t + j), 0, SUB, y0)
        ready = SUB * j - 2 if j < LD else PLANES
        if j and carry is None:
            zero = jnp.zeros((CY, NZ), jnp.float32)
            carry = (image_plane(0), image_plane(1)) + (zero,) * 4
        for p in range(done, ready):
            carry = sum_plane(p, carry)
        done = max(done, ready)
        if j < LD:
            keep(charge, SUB, 2 + SUB * j)
            for p in range(SUB * j, SUB * j + SUB):
                load_plane(p)
    lane = lax.broadcasted_iota(jnp.int32, (1, 128), 1)
    line = jnp.zeros((1, 128), jnp.float32)
    for i, total in enumerate(carry[2:]):
        line = line + jnp.where(lane == i, jnp.sum(total), 0.0)
    for d in range(NE * NK):
        sums[d] = line


def fields(e, k, volts, occ, cells, corners, fixed, gate, xlow, xhigh, ylow, yhigh):
    whole = lambda x: pl.BlockSpec(x.shape, lambda i, *_: (0,) * x.ndim)
    shapes = [
        jax.ShapeDtypeStruct((NE * NK, 1, 128), jnp.float32),
        jax.ShapeDtypeStruct((2, PLANES, CY, NZ), jnp.float32),
    ]
    return pl.pallas_call(
        field_body,
        grid_spec=pltpu.PrefetchScalarGridSpec(
            num_scalar_prefetch=2,
            grid=(1,),
            in_specs=[whole(x) for x in (occ, cells, corners, xlow, xhigh, ylow, yhigh)]
            + [pl.BlockSpec(memory_space=pltpu.HBM)] * 3,
            out_specs=[
                pl.BlockSpec((NE * NK, 1, 128), lambda i, *_: (0, 0, 0)),
                pl.BlockSpec((2, PLANES, CY, NZ), lambda i, *_: (0, 0, 0, 0)),
            ],
            scratch_shapes=[
                pltpu.VMEM((PLANES + 4, W, NZ), jnp.float32),
                pltpu.VMEM((PLANES + 4, W, NZ), jnp.float32),
                pltpu.VMEM((PLANES, CY, NZ), jnp.float32),
                pltpu.VMEM((PLANES, CY, NZ), jnp.int32),
                pltpu.SMEM((PLANES,), jnp.float32),
                pltpu.SemaphoreType.DMA((3,)),
            ],
        ),
        out_shape=shapes,
        compiler_params=params(16),
        name="fields",
    )(e[None], k[None], occ, cells, corners, xlow, xhigh, ylow, yhigh, in_hbm(volts), in_hbm(fixed), in_hbm(gate))


def lengths(sums):
    line = jnp.sum(sums[...].reshape(NE * NK, 128), axis=0, keepdims=True)
    lane = lax.broadcasted_iota(jnp.int32, (1, 128), 1)
    rr, rw, ww, waw = [
        jnp.broadcast_to(jnp.sum(jnp.where(lane == i, line, 0.0), axis=1, keepdims=True), (1, NZ)) for i in range(4)
    ]
    alpha = rr / rw
    norm = alpha * alpha * ww - rr
    ratio = norm / rr
    ahead = 1.0 + ratio
    curve = ahead * ahead * rw - 2.0 * ahead * alpha * ww + alpha * alpha * waw
    small = (norm <= 1e-9 * rr) | (curve <= 0.0)
    step = jnp.where(small, alpha, norm / curve)
    ahead = jnp.where(small, 1.0, ahead)
    return alpha + step * ahead, -alpha * step


def pick_body(kpt, sums, cells_near, rw, out, grid_out, grid_here, leaving):
    y0 = kpt[0] * CY
    wide = 2 * COL
    counts = counting(NZ)
    c_r, c_w = [jnp.broadcast_to(c, (SUB * CY, NZ)) for c in lengths(sums)]
    copies = []
    for j in range(LD):
        at = pl.ds(SUB * j, SUB)
        field = c_r * rw[0, at].reshape(SUB * CY, NZ) + c_w * rw[1, at].reshape(SUB * CY, NZ)
        grid_here[at] = field.reshape(SUB, CY, NZ)
        copies.append(pltpu.make_async_copy(grid_here.at[at], grid_out.at[at], leaving.at[j]))
        copies[-1].start()
        high, low = split_parts(field)
        for n in range(ORB // wide):
            cells = cells_near[LD + j : LD + j + 1, n * wide : (n + 1) * wide]
            dy = ((cells >> 8) & (NY - 1)) - y0
            row = jnp.where((dy >= 0) & (dy < CY), (cells >> 15) * CY + dy, -1)
            z = cells & (NZ - 1)
            right = marks(z.astype(jnp.float32), NZ, counts)
            lines = jnp.dot(high, right, preferred_element_type=jnp.float32)
            lines = lines + jnp.dot(low, right, preferred_element_type=jnp.float32)
            hit = lax.broadcasted_iota(jnp.int32, (SUB * CY, wide), 0) == row
            value = jnp.sum(jnp.where(hit, lines, 0.0), axis=0, keepdims=True)
            for h in range(2):
                out[2 * n + h, j : j + 1, :] = value[:, h * COL : (h + 1) * COL]
    for copy in copies:
        copy.wait()


def pick(k, sums, cells, rw):
    whole = lambda shape: pl.BlockSpec(shape, lambda i, *_: (0,) * len(shape))
    shape = jax.ShapeDtypeStruct((NK, LD, COL), jnp.float32)
    return pl.pallas_call(
        pick_body,
        grid_spec=pltpu.PrefetchScalarGridSpec(
            num_scalar_prefetch=1,
            grid=(1,),
            in_specs=[whole(sums.shape), whole(cells.shape), whole(rw.shape)],
            out_specs=[whole(shape.shape), pl.BlockSpec(memory_space=pltpu.HBM)],
            scratch_shapes=[pltpu.VMEM((PLANES, CY, NZ), jnp.float32), pltpu.SemaphoreType.DMA((LD,))],
        ),
        out_shape=[shape, pltpu.HBM((PLANES, CY, NZ), jnp.float32)],
        compiler_params=params(12),
        name="pick",
    )(k[None], sums, cells, rw)


def join_body(picked, out):
    total = picked[0]
    for i in range(1, NK):
        total = total + picked[i]
    for d in range(NE * NZC):
        out[d] = total


def join(picked):
    return pl.pallas_call(
        join_body,
        out_shape=jax.ShapeDtypeStruct((NE * NZC, LD, COL), jnp.float32),
        compiler_params=params(4),
        name="join",
    )(picked)


def band_body(which, density, values, before, out):
    totals = [[None] * (NE // 2) for _ in range(EL)]
    for m in range(NE // 2):
        for z in range(NZC):
            start = pl.multiple_of((2 * z + which[0]) * COL, 128)
            v = values[2 * m : 2 * m + 2, z].reshape(16, COL)
            for i in range(EL):
                part = density[i, 16 * m : 16 * m + 16, pl.ds(start, COL)].astype(jnp.float32) * v
                for t in range(TL):
                    tile = part[:, 128 * t : 128 * (t + 1)]
                    totals[i][m] = tile if totals[i][m] is None else totals[i][m] + tile
    for i in range(EL):
        total = jnp.concatenate(totals[i], axis=0)
        out[i : i + 1, :] = before[i : i + 1, :] + jnp.sum(total.T, axis=0, keepdims=True) * ORB**-0.5


def band(which, density, values, before):
    whole = lambda x: pl.BlockSpec(x.shape, lambda i, *_: (0,) * x.ndim)
    return pl.pallas_call(
        band_body,
        grid_spec=pltpu.PrefetchScalarGridSpec(
            num_scalar_prefetch=1,
            grid=(1,),
            in_specs=[whole(density), whole(values), whole(before)],
            out_specs=whole(before),
        ),
        out_shape=jax.ShapeDtypeStruct((EL, LAYERS), jnp.float32),
        compiler_params=params(8),
        name="band",
    )(which, density, values, before)


def shift_up(x, axis):
    return lax.ppermute(x, axis, [(i, i + 1) for i in range(lax.axis_size(axis) - 1)])


def shift_down(x, axis):
    return lax.ppermute(x, axis, [(i + 1, i) for i in range(lax.axis_size(axis) - 1)])


def one_step(density, quad_weights, orbital_cells, fixed_charge, gate_mask, gate_voltage):
    e = lax.axis_index(ENERGY).astype(jnp.int32)
    k = lax.axis_index(KPT).astype(jnp.int32)
    core = lax.axis_index(CORE).astype(jnp.int32)[None]
    density = density.reshape(EL, LAYERS, ORB)

    own, other = occupancy_parts(e, k, gate_voltage, quad_weights.reshape(1, EL), density, fixed_charge, gate_mask)
    chips = NE * NZC
    received = swap_cores(other.reshape(chips, 32, 128))
    xup, xdown, yup, ydown, cells = edges(e, gate_voltage, fixed_charge, gate_mask, orbital_cells)
    pair = own.reshape(chips, 32, 128) + received
    parts = exchange(pair, CHIPS)
    xlow = shift_up(xup, ENERGY)
    xhigh = shift_down(xdown, ENERGY)
    ylow = shift_up(yup, KPT)
    yhigh = shift_down(ydown, KPT)
    parts, xlow, xhigh = lax.optimization_barrier((parts, xlow, xhigh))
    occ, corners = collect(e, k, parts)
    occ = exchange(occ, KPT)
    sums, rw = fields(
        e, k, gate_voltage, occ, cells, corners, fixed_charge, gate_mask, xlow, xhigh, ylow, yhigh
    )
    all_sums = exchange(sums, EVERY)
    picked, potential = pick(k, all_sums, cells, rw)
    picked = exchange(picked, KPT)
    same = exchange(join(picked), CHIPS)
    shape = (NE, NZC, LD, COL)
    cross = swap_cores(same)
    shift = band(core, density, same.reshape(shape), jnp.zeros((EL, LAYERS), jnp.float32))
    shift = band(1 - core, density, cross.reshape(shape), shift)
    return potential, shift.reshape(EL, 1, LAYERS)


def solution(mesh):
    split = Mesh(mesh.devices.reshape(4, 4, 4, 2), ("energy_0", "energy_1", "kpt_0", "kpt_1"))
    in_specs = (
        P(ENERGY, KPT, None, None),
        P(ENERGY, KPT),
        P(),
        P(ENERGY, KPT, None),
        P(ENERGY, KPT, None),
        P(ENERGY),
    )
    out_specs = (P(ENERGY, KPT, None), P(ENERGY, KPT, None))
    return jax.shard_map(one_step, mesh=split, in_specs=in_specs, out_specs=out_specs, check_vma=False)
```

```python
import jax
import jax.numpy as jnp
from jax import lax
from jax.experimental import pallas as pl
from jax.experimental.pallas import tpu as pltpu
from jax.sharding import Mesh
from jax.sharding import PartitionSpec as P

ENERGY = ("energy_0", "energy_1")
KPT = ("kpt_0", "kpt_1")
CHIPS = ("energy_0", "energy_1", "kpt_0")
CORE = "kpt_1"
EVERY = ("energy_0", "energy_1", "kpt_0", "kpt_1")

NE = 16
NK = 8
NZC = 4
SUB = 8
LAYERS = 128
LD = 8
ORB = 3072
CY = 16
NY = 128
NZ = 256
PLANES = 64
EL = 4
W = 24
WC = 20
COL = ORB // NK
TL = COL // 128
PENALTY = 4.0
PIECES = 8
AHEAD = 4


def swap_cores(x):
    return lax.ppermute(x, CORE, [(0, 1), (1, 0)])


def exchange(x, axis):
    return lax.all_to_all(x, axis, split_axis=0, concat_axis=0, tiled=True)


def in_hbm(x):
    return pltpu.with_memory_space_constraint(x, pltpu.HBM)


def params(mib):
    return pltpu.CompilerParams(vmem_limit_bytes=mib * 1024 * 1024)


def occupancy_body(energy, kpt, weights_out, density_out, volts_out, fixed, gate, own, other,
                   weights, density, fixed_ends, gate_ends, volts, arrivals, blocks):
    e = energy[0]
    k = kpt[0]
    core = k % 2
    small = [
        pltpu.make_async_copy(weights_out, weights, arrivals.at[0]),
        pltpu.make_async_copy(volts_out, volts, arrivals.at[1]),
    ]
    for i, plane in enumerate((0, PLANES - 1)):
        small.append(pltpu.make_async_copy(fixed.at[plane], fixed_ends.at[i], arrivals.at[2 + 2 * i]))
        small.append(pltpu.make_async_copy(gate.at[plane], gate_ends.at[i], arrivals.at[3 + 2 * i]))
    large = [
        pltpu.make_async_copy(density_out.at[:, :, pl.ds(2 * COL * z, 2 * COL)], density.at[z], blocks.at[z])
        for z in range(NZC)
    ]
    for copy in small[:1] + large[:AHEAD] + small[1:]:
        copy.start()
    small[0].wait()
    scale = [jnp.broadcast_to(weights[0:1, n : n + 1], (16, COL)) for n in range(EL)]
    zero = jnp.zeros((3, 128), jnp.float32)
    for z in range(NZC):
        large[z].wait()
        if z + AHEAD < NZC:
            large[z + AHEAD].start()
        for half, out in ((0, own), (1, other)):
            which = core if half == 0 else 1 - core
            start = pl.multiple_of(which * COL, 128)
            for i in range(0, NE, 2):
                total = None
                for n in range(EL):
                    part = density[z, n, 8 * i : 8 * i + 16, pl.ds(start, COL)].astype(jnp.float32) * scale[n]
                    total = part if total is None else total + part
                for h in range(2):
                    at = i + h
                    for t in range(TL):
                        tile = total[8 * h : 8 * h + 8, 128 * t : 128 * (t + 1)]
                        out[at, z, 8 * t : 8 * t + 8, :] = tile
                        if at + 1 < NE:
                            out[at + 1, z, 24 + t : 25 + t, :] = tile[7:8]
                        if at > 0:
                            out[at - 1, z, 27 + t : 28 + t, :] = tile[0:1]
            out[0, z, 24:27, :] = zero
            out[NE - 1, z, 27:30, :] = zero
            for i in range(NE):
                out[i, z, 30:32, :] = zero[:2]
    for copy in small[1:]:
        copy.wait()

    for dx in (-1, 1):
        for dy in (-1, 1):
            to_e = e + dx
            to_k = k + dy

            @pl.when((to_e >= 0) & (to_e < NE) & (to_k >= 0) & (to_k < NK))
            def _(dx=dx, dy=dy, to_e=to_e, to_k=to_k):
                i = 1 if dx == 1 else 0
                y = CY - 1 if dy == 1 else 0
                g = gate_ends[i, y : y + 1, :].astype(jnp.float32)
                line = fixed_ends[i, y : y + 1, :] + PENALTY * g * volts[(PLANES - 1) * i]
                other[to_e, to_k // 2, 30:31, :] = line[:, :128]
                other[to_e, to_k // 2, 31:32, :] = line[:, 128:]


def occupancy_parts(e, k, volts, weights, density, fixed, gate):
    shape = (NE, NZC, 32, 128)
    hbm = pl.BlockSpec(memory_space=pltpu.HBM)
    return pl.pallas_call(
        occupancy_body,
        grid_spec=pltpu.PrefetchScalarGridSpec(
            num_scalar_prefetch=2,
            grid=(1,),
            in_specs=[hbm] * 5,
            out_specs=[pl.BlockSpec(shape, lambda i, *_: (0, 0, 0, 0))] * 2,
            scratch_shapes=[
                pltpu.VMEM((1, EL), jnp.float32),
                pltpu.VMEM((NZC, EL, LAYERS, 2 * COL), jnp.bfloat16),
                pltpu.VMEM((2, CY, NZ), jnp.float32),
                pltpu.VMEM((2, CY, NZ), jnp.int32),
                pltpu.SMEM((PLANES,), jnp.float32),
                pltpu.SemaphoreType.DMA((6,)),
                pltpu.SemaphoreType.DMA((NZC,)),
            ],
        ),
        out_shape=[jax.ShapeDtypeStruct(shape, jnp.float32)] * 2,
        compiler_params=params(10),
        name="occupancy_parts",
    )(e[None], k[None], in_hbm(weights), in_hbm(density), in_hbm(volts), in_hbm(fixed), in_hbm(gate))


def edges_body(energy, volts_out, fixed, gate, cells, xup, xdown, yup, ydown, near, fixed_here, gate_here, volts, arrivals):
    copies = [
        pltpu.make_async_copy(volts_out, volts, arrivals.at[2]),
        pltpu.make_async_copy(fixed, fixed_here, arrivals.at[0]),
        pltpu.make_async_copy(gate, gate_here, arrivals.at[1]),
    ]
    later = []
    for n in range(3):
        start = pl.multiple_of(jnp.clip(energy[0] + n - 1, 0, NE - 1) * LD, LD)
        later.append(
            pltpu.make_async_copy(cells.at[pl.ds(start, LD)], near.at[pl.ds(n * LD, LD)], arrivals.at[3 + n])
        )
    for copy in copies + later:
        copy.start()
    for copy in copies:
        copy.wait()
    for out, planes in ((xup, (PLANES - 2, PLANES - 1)), (xdown, (0, 1))):
        for i, p in enumerate(planes):
            g = gate_here[p].astype(jnp.float32)
            out[i] = fixed_here[p] + PENALTY * g * volts[p]
            if p in (0, PLANES - 1):
                out[2] = g

    def one_plane(p, carry):
        volt = PENALTY * volts[p]
        for out, rows in ((yup, (CY - 2, CY - 1)), (ydown, (0, 1))):
            for i, y in enumerate(rows):
                g = gate_here[p, y : y + 1, :].astype(jnp.float32)
                out[i, pl.ds(p, 1), :] = fixed_here[p, y : y + 1, :] + volt * g
                if y in (0, CY - 1):
                    out[2, pl.ds(p, 1), :] = g
        return carry

    lax.fori_loop(0, PLANES, one_plane, 0, unroll=8)
    for copy in later:
        copy.wait()


def edges(e, volts, fixed, gate, cells):
    shapes = [(3, CY, NZ)] * 2 + [(3, PLANES, NZ)] * 2
    hbm = pl.BlockSpec(memory_space=pltpu.HBM)
    return pl.pallas_call(
        edges_body,
        grid_spec=pltpu.PrefetchScalarGridSpec(
            num_scalar_prefetch=1,
            grid=(1,),
            in_specs=[hbm, hbm, hbm, hbm],
            out_specs=[pl.BlockSpec(x, lambda i, *_: (0, 0, 0)) for x in shapes]
            + [pl.BlockSpec((3 * LD, ORB), lambda i, *_: (0, 0))],
            scratch_shapes=[
                pltpu.VMEM((PLANES, CY, NZ), jnp.float32),
                pltpu.VMEM((PLANES, CY, NZ), jnp.int32),
                pltpu.SMEM((PLANES,), jnp.float32),
                pltpu.SemaphoreType.DMA((6,)),
            ],
        ),
        out_shape=[jax.ShapeDtypeStruct(x, jnp.float32) for x in shapes]
        + [jax.ShapeDtypeStruct((3 * LD, ORB), jnp.int32)],
        compiler_params=params(8),
        name="edges",
    )(e[None], in_hbm(volts), in_hbm(fixed), in_hbm(gate), in_hbm(cells))


def pair_body(own, received, out, here, leaving):
    copies = []
    cut = NE * NZC // PIECES
    for i in range(PIECES):
        at = pl.ds(cut * i, cut)
        here[at] = own[at] + received[at]
        copies.append(pltpu.make_async_copy(here.at[at], out.at[at], leaving.at[i]))
        copies[-1].start()
    for copy in copies:
        copy.wait()


def add_pair(own, received):
    whole = pl.BlockSpec(own.shape, lambda i: (0, 0, 0))
    return pl.pallas_call(
        pair_body,
        grid_spec=pltpu.PrefetchScalarGridSpec(
            num_scalar_prefetch=0,
            grid=(1,),
            in_specs=[whole, whole],
            out_specs=pl.BlockSpec(memory_space=pltpu.HBM),
            scratch_shapes=[pltpu.VMEM(own.shape, jnp.float32), pltpu.SemaphoreType.DMA((PIECES,))],
        ),
        out_shape=pltpu.HBM(own.shape, jnp.float32),
        compiler_params=params(4),
        name="add_pair",
    )(own, received)


def collect_body(energy, kpt, parts, out, corners):
    e = energy[0]
    k = kpt[0]
    total = parts[0]
    for i in range(1, NE * NZC):
        total = total + parts[i]
    for n in range(NK):
        out[n] = total
    for i, dx in enumerate((-1, 1)):
        for j, dy in enumerate((-1, 1)):
            from_e = e + dx
            from_k = k + dy
            there = (from_e >= 0) & (from_e < NE) & (from_k >= 0) & (from_k < NK)
            source = jnp.where(there, from_e * NZC + from_k // 2, 0)
            lines = parts[source, 30:32, :]
            corners[i, j : j + 1, 0:128] = jnp.where(there, lines[0:1], 0.0)
            corners[i, j : j + 1, 128:256] = jnp.where(there, lines[1:2], 0.0)


def collect(e, k, parts):
    whole = lambda shape: pl.BlockSpec(shape, lambda i, *_: (0, 0, 0))
    shapes = [(NK, 32, 128), (2, 2, NZ)]
    return pl.pallas_call(
        collect_body,
        grid_spec=pltpu.PrefetchScalarGridSpec(
            num_scalar_prefetch=2,
            grid=(1,),
            in_specs=[whole((NE * NZC, 32, 128))],
            out_specs=[whole(x) for x in shapes],
        ),
        out_shape=[jax.ShapeDtypeStruct(x, jnp.float32) for x in shapes],
        compiler_params=params(4),
        name="collect",
    )(e[None], k[None], parts)


def split_parts(x):
    high = x.astype(jnp.bfloat16)
    low = (x - high.astype(jnp.float32)).astype(jnp.bfloat16)
    return high, low


def spread(line, rows):
    block = jnp.broadcast_to(line, (16, 128)).astype(jnp.bfloat16)
    return jnp.concatenate([block] * (rows // 16), axis=0)


def counting(rows):
    return lax.broadcasted_iota(jnp.int32, (rows, 128), 0).astype(jnp.float32).astype(jnp.bfloat16)


def tiles_of(line):
    return [line[:, 128 * t : 128 * (t + 1)] for t in range(line.shape[1] // 128)]


def marks(index, rows, counts):
    one = jnp.ones((), jnp.bfloat16)
    zero = jnp.zeros((), jnp.bfloat16)
    return jnp.concatenate([jnp.where(counts[:rows] == spread(t, rows), one, zero) for t in tiles_of(index)], axis=1)


def charge_of(cells, values, first_plane, planes, y0):
    plane = (cells >> 15) - first_plane
    dy = ((cells >> 8) & (NY - 1)) - y0
    near = (dy >= -2) & (dy < CY + 2) & (plane >= 0) & (plane < planes)
    row = jnp.where(near, plane * WC + jnp.where(dy >= 0, dy, dy + WC), -1).astype(jnp.float32)
    z = (cells & (NZ - 1)).astype(jnp.float32)
    rows = planes * WC
    padded = -(-rows // 16) * 16
    counts = counting(NZ)
    high = values.astype(jnp.bfloat16).astype(jnp.float32)
    low = values - high
    zero = jnp.zeros((), jnp.bfloat16)
    tops, bottoms = [], []
    for t, h, l in zip(tiles_of(row), tiles_of(high), tiles_of(low)):
        hit = counts[:padded] == spread(t, padded)
        tops.append(jnp.where(hit, spread(h, padded), zero))
        bottoms.append(jnp.where(hit, spread(l, padded), zero))
    left = jnp.concatenate([jnp.concatenate(tops, axis=1), jnp.concatenate(bottoms, axis=1)], axis=0)
    right = marks(z, NZ, counts)
    both = lax.dot_general(left, right, (((1,), (1,)), ((), ())), preferred_element_type=jnp.float32)
    return both[:padded] + both[padded:]


def in_plane(here):
    lane = lax.broadcasted_iota(jnp.int32, (W, NZ), 1)
    total = pltpu.roll(here, 1, 0) + pltpu.roll(here, W - 1, 0)
    total = total + jnp.where(lane == 0, 0.0, pltpu.roll(here, 1, 1))
    return total + jnp.where(lane == NZ - 1, 0.0, pltpu.roll(here, NZ - 1, 1))


def field_body(energy, kpt, occ, cells, corners, xlow, xhigh, ylow, yhigh, volts_out, fixed, gate,
               sums, fields_out, r_ext, g_ext, fixed_here, gate_here, volts, arrivals):
    e = energy[0]
    k = kpt[0]
    y0 = k * CY
    copies = [
        pltpu.make_async_copy(volts_out, volts, arrivals.at[2]),
        pltpu.make_async_copy(fixed, fixed_here, arrivals.at[0]),
        pltpu.make_async_copy(gate, gate_here, arrivals.at[1]),
    ]
    for copy in copies:
        copy.start()
    row = lax.broadcasted_iota(jnp.int32, (W, NZ), 0)
    y = jnp.where(row < CY + 4, row, row - W) + y0
    valid = jnp.where((y >= 0) & (y < NY), 1.0, 0.0)

    def values_of(index):
        return jnp.concatenate(
            [occ[c, pl.ds(index(t), 1), :] for c in range(NK) for t in range(TL)], axis=1
        )

    gap = jnp.zeros((4, NZ), jnp.float32)

    def keep(charge, planes, at):
        for p in range(planes):
            r_ext[at + p, 0:CY, :] = -charge[WC * p : WC * p + CY]
            r_ext[at + p, CY : CY + 2, :] = -charge[WC * p + CY : WC * p + CY + 2]
            r_ext[at + p, CY + 2 : W - 2, :] = gap
            r_ext[at + p, W - 2 : W, :] = -charge[WC * p + CY + 2 : WC * p + WC]

    keep(charge_of(cells[LD - 1 : LD, :], values_of(lambda t: 24 + t), SUB - 2, 2, y0), 2, 0)
    sub = lax.broadcasted_iota(jnp.int32, (8, NZ), 0)
    none = jnp.zeros((8, NZ), jnp.float32)
    wide = lambda x: jnp.broadcast_to(x, (8, NZ))

    def outside(at, halo, i):
        for n in range(2):
            r_ext[at + n, 0:CY, :] = r_ext[at + n, 0:CY, :] + halo[n]
        beside = at + 1 - i
        tile = jnp.where(sub == 0, wide(corners[i, 1:2, :]), jnp.where(sub == 7, wide(corners[i, 0:1, :]), none))
        g_ext[beside, 0:CY, :] = halo[2]
        r_ext[beside, CY:W, :] = r_ext[beside, CY:W, :] + tile
        g_ext[beside, CY:W, :] = none

    outside(0, xlow, 0)

    def load_plane(p):
        at = slice(p, p + 1)
        g = gate_here[p].astype(jnp.float32)
        g_ext[p + 2, 0:CY, :] = g
        r_ext[p + 2, 0:CY, :] = r_ext[p + 2, 0:CY, :] + (fixed_here[p] + PENALTY * g * volts[p])
        tile = jnp.where(sub == 0, wide(yhigh[0, at, :]), jnp.where(sub == 1, wide(yhigh[1, at, :]), none))
        tile = jnp.where(sub == 6, wide(ylow[0, at, :]), jnp.where(sub == 7, wide(ylow[1, at, :]), tile))
        r_ext[p + 2, CY:W, :] = r_ext[p + 2, CY:W, :] + tile
        tile = jnp.where(sub == 0, wide(yhigh[2, at, :]), jnp.where(sub == 7, wide(ylow[2, at, :]), none))
        g_ext[p + 2, CY:W, :] = tile

    def image_plane(p):
        here = r_ext[p + 1]
        inside = valid
        if p in (0, PLANES + 1):
            x = e * PLANES + p - 1
            inside = valid * jnp.where((x >= 0) & (x < NE * PLANES), 1.0, 0.0)
        around = r_ext[p + 2] + r_ext[p] + in_plane(here)
        return ((6.0 + PENALTY * g_ext[p + 1]) * here - around) * inside

    def sum_plane(p, carry):
        before, here, rr, rw, ww, waw = carry
        after = image_plane(p + 2)
        r = r_ext[p + 2, 0:CY, :]
        w = here[0:CY]
        image = ((6.0 + PENALTY * g_ext[p + 2]) * here - (before + after + in_plane(here)))[0:CY]
        fields_out[0, p] = r
        fields_out[1, p] = w
        return here, after, rr + r * r, rw + r * w, ww + w * w, waw + w * image

    carry = None
    done = 0
    for j in range(LD + 1):
        if j < LD:
            charge = charge_of(cells[LD + j : LD + j + 1, :], values_of(lambda t: 8 * t + j), 0, SUB, y0)
        else:
            charge = charge_of(cells[2 * LD : 2 * LD + 1, :], values_of(lambda t: 27 + t), 0, 2, y0)
        if j == 0:
            for copy in copies:
                copy.wait()
        ready = SUB * j - 2
        if j and carry is None:
            zero = jnp.zeros((CY, NZ), jnp.float32)
            carry = (image_plane(0), image_plane(1)) + (zero,) * 4
        for p in range(done, ready):
            carry = sum_plane(p, carry)
        done = max(done, ready)
        if j < LD:
            keep(charge, SUB, 2 + SUB * j)
            for p in range(SUB * j, SUB * j + SUB):
                load_plane(p)
    keep(charge, 2, PLANES + 2)
    outside(PLANES + 2, xhigh, 1)
    for p in range(done, PLANES):
        carry = sum_plane(p, carry)
    lane = lax.broadcasted_iota(jnp.int32, (1, 128), 1)
    line = jnp.zeros((1, 128), jnp.float32)
    for i, total in enumerate(carry[2:]):
        line = line + jnp.where(lane == i, jnp.sum(total), 0.0)
    for d in range(NE * NK):
        sums[d] = line


def fields(e, k, volts, occ, cells, corners, fixed, gate, xlow, xhigh, ylow, yhigh):
    whole = lambda x: pl.BlockSpec(x.shape, lambda i, *_: (0,) * x.ndim)
    shapes = [
        jax.ShapeDtypeStruct((NE * NK, 1, 128), jnp.float32),
        jax.ShapeDtypeStruct((2, PLANES, CY, NZ), jnp.float32),
    ]
    return pl.pallas_call(
        field_body,
        grid_spec=pltpu.PrefetchScalarGridSpec(
            num_scalar_prefetch=2,
            grid=(1,),
            in_specs=[whole(x) for x in (occ, cells, corners, xlow, xhigh, ylow, yhigh)]
            + [pl.BlockSpec(memory_space=pltpu.HBM)] * 3,
            out_specs=[
                pl.BlockSpec((NE * NK, 1, 128), lambda i, *_: (0, 0, 0)),
                pl.BlockSpec((2, PLANES, CY, NZ), lambda i, *_: (0, 0, 0, 0)),
            ],
            scratch_shapes=[
                pltpu.VMEM((PLANES + 4, W, NZ), jnp.float32),
                pltpu.VMEM((PLANES + 4, W, NZ), jnp.float32),
                pltpu.VMEM((PLANES, CY, NZ), jnp.float32),
                pltpu.VMEM((PLANES, CY, NZ), jnp.int32),
                pltpu.SMEM((PLANES,), jnp.float32),
                pltpu.SemaphoreType.DMA((3,)),
            ],
        ),
        out_shape=shapes,
        compiler_params=params(16),
        name="fields",
    )(e[None], k[None], occ, cells, corners, xlow, xhigh, ylow, yhigh, in_hbm(volts), in_hbm(fixed), in_hbm(gate))


def lengths(sums):
    line = jnp.sum(sums[...].reshape(NE * NK, 128), axis=0, keepdims=True)
    lane = lax.broadcasted_iota(jnp.int32, (1, 128), 1)
    rr, rw, ww, waw = [
        jnp.broadcast_to(jnp.sum(jnp.where(lane == i, line, 0.0), axis=1, keepdims=True), (1, NZ)) for i in range(4)
    ]
    alpha = rr / rw
    norm = alpha * alpha * ww - rr
    ratio = norm / rr
    ahead = 1.0 + ratio
    curve = ahead * ahead * rw - 2.0 * ahead * alpha * ww + alpha * alpha * waw
    small = (norm <= 1e-9 * rr) | (curve <= 0.0)
    step = jnp.where(small, alpha, norm / curve)
    ahead = jnp.where(small, 1.0, ahead)
    return alpha + step * ahead, -alpha * step


def pick_body(kpt, sums, cells_near, rw, out, grid_out, grid_here, leaving):
    y0 = kpt[0] * CY
    wide = 2 * COL
    counts = counting(NZ)
    c_r, c_w = [jnp.broadcast_to(c, (SUB * CY, NZ)) for c in lengths(sums)]
    copies = []
    for j in range(LD):
        at = pl.ds(SUB * j, SUB)
        field = c_r * rw[0, at].reshape(SUB * CY, NZ) + c_w * rw[1, at].reshape(SUB * CY, NZ)
        grid_here[at] = field.reshape(SUB, CY, NZ)
        copies.append(pltpu.make_async_copy(grid_here.at[at], grid_out.at[at], leaving.at[j]))
        copies[-1].start()
        high, low = split_parts(field)
        for n in range(ORB // wide):
            cells = cells_near[LD + j : LD + j + 1, n * wide : (n + 1) * wide]
            dy = ((cells >> 8) & (NY - 1)) - y0
            row = jnp.where((dy >= 0) & (dy < CY), (cells >> 15) * CY + dy, -1)
            z = cells & (NZ - 1)
            right = marks(z.astype(jnp.float32), NZ, counts)
            lines = jnp.dot(high, right, preferred_element_type=jnp.float32)
            lines = lines + jnp.dot(low, right, preferred_element_type=jnp.float32)
            hit = lax.broadcasted_iota(jnp.int32, (SUB * CY, wide), 0) == row
            value = jnp.sum(jnp.where(hit, lines, 0.0), axis=0, keepdims=True)
            for h in range(2):
                out[2 * n + h, j : j + 1, :] = value[:, h * COL : (h + 1) * COL]
    for copy in copies:
        copy.wait()


def pick(k, sums, cells, rw):
    whole = lambda shape: pl.BlockSpec(shape, lambda i, *_: (0,) * len(shape))
    shape = jax.ShapeDtypeStruct((NK, LD, COL), jnp.float32)
    return pl.pallas_call(
        pick_body,
        grid_spec=pltpu.PrefetchScalarGridSpec(
            num_scalar_prefetch=1,
            grid=(1,),
            in_specs=[whole(sums.shape), whole(cells.shape), whole(rw.shape)],
            out_specs=[whole(shape.shape), pl.BlockSpec(memory_space=pltpu.HBM)],
            scratch_shapes=[pltpu.VMEM((PLANES, CY, NZ), jnp.float32), pltpu.SemaphoreType.DMA((LD,))],
        ),
        out_shape=[shape, pltpu.HBM((PLANES, CY, NZ), jnp.float32)],
        compiler_params=params(12),
        name="pick",
    )(k[None], sums, cells, rw)


def join_body(picked, out):
    total = picked[0]
    for i in range(1, NK):
        total = total + picked[i]
    for d in range(NE * NZC):
        out[d] = total


def join(picked):
    return pl.pallas_call(
        join_body,
        out_shape=jax.ShapeDtypeStruct((NE * NZC, LD, COL), jnp.float32),
        compiler_params=params(4),
        name="join",
    )(picked)


def band_body(which, density, values, before, out):
    totals = [[None] * (NE // 2) for _ in range(EL)]
    for m in range(NE // 2):
        for z in range(NZC):
            start = pl.multiple_of((2 * z + which[0]) * COL, 128)
            v = values[2 * m : 2 * m + 2, z].reshape(16, COL)
            for i in range(EL):
                part = density[i, 16 * m : 16 * m + 16, pl.ds(start, COL)].astype(jnp.float32) * v
                for t in range(TL):
                    tile = part[:, 128 * t : 128 * (t + 1)]
                    totals[i][m] = tile if totals[i][m] is None else totals[i][m] + tile
    for i in range(EL):
        total = jnp.concatenate(totals[i], axis=0)
        out[i : i + 1, :] = before[i : i + 1, :] + jnp.sum(total.T, axis=0, keepdims=True) * ORB**-0.5


def band(which, density, values, before):
    whole = lambda x: pl.BlockSpec(x.shape, lambda i, *_: (0,) * x.ndim)
    return pl.pallas_call(
        band_body,
        grid_spec=pltpu.PrefetchScalarGridSpec(
            num_scalar_prefetch=1,
            grid=(1,),
            in_specs=[whole(density), whole(values), whole(before)],
            out_specs=whole(before),
        ),
        out_shape=jax.ShapeDtypeStruct((EL, LAYERS), jnp.float32),
        compiler_params=params(8),
        name="band",
    )(which, density, values, before)


def shift_up(x, axis):
    return lax.ppermute(x, axis, [(i, i + 1) for i in range(lax.axis_size(axis) - 1)])


def shift_down(x, axis):
    return lax.ppermute(x, axis, [(i + 1, i) for i in range(lax.axis_size(axis) - 1)])


def one_step(density, quad_weights, orbital_cells, fixed_charge, gate_mask, gate_voltage):
    e = lax.axis_index(ENERGY).astype(jnp.int32)
    k = lax.axis_index(KPT).astype(jnp.int32)
    core = lax.axis_index(CORE).astype(jnp.int32)[None]
    density = density.reshape(EL, LAYERS, ORB)

    own, other = occupancy_parts(e, k, gate_voltage, quad_weights.reshape(1, EL), density, fixed_charge, gate_mask)
    chips = NE * NZC
    received = swap_cores(other.reshape(chips, 32, 128))
    xup, xdown, yup, ydown, cells = edges(e, gate_voltage, fixed_charge, gate_mask, orbital_cells)
    pair = add_pair(own.reshape(chips, 32, 128), received)
    parts = exchange(pair, CHIPS)
    xlow = shift_up(xup, ENERGY)
    xhigh = shift_down(xdown, ENERGY)
    ylow = shift_up(yup, KPT)
    yhigh = shift_down(ydown, KPT)
    parts, xlow, xhigh = lax.optimization_barrier((parts, xlow, xhigh))
    occ, corners = collect(e, k, parts)
    occ = exchange(occ, KPT)
    sums, rw = fields(
        e, k, gate_voltage, occ, cells, corners, fixed_charge, gate_mask, xlow, xhigh, ylow, yhigh
    )
    all_sums = exchange(sums, EVERY)
    picked, potential = pick(k, all_sums, cells, rw)
    picked = exchange(picked, KPT)
    same = exchange(join(picked), CHIPS)
    shape = (NE, NZC, LD, COL)
    cross = swap_cores(same)
    shift = band(core, density, same.reshape(shape), jnp.zeros((EL, LAYERS), jnp.float32))
    shift = band(1 - core, density, cross.reshape(shape), shift)
    return potential, shift.reshape(EL, 1, LAYERS)


def solution(mesh):
    split = Mesh(mesh.devices.reshape(4, 4, 4, 2), ("energy_0", "energy_1", "kpt_0", "kpt_1"))
    in_specs = (
        P(ENERGY, KPT, None, None),
        P(ENERGY, KPT),
        P(),
        P(ENERGY, KPT, None),
        P(ENERGY, KPT, None),
        P(ENERGY),
    )
    out_specs = (P(ENERGY, KPT, None), P(ENERGY, KPT, None))
    return jax.shard_map(one_step, mesh=split, in_specs=in_specs, out_specs=out_specs, check_vma=False)
```
